32 devices in a mesh: dp: 8 (over y, x, core), seq: 4 (over z).
Axes of the slice: x: 2, y: 2, z: 4, core: 2. Of those that a mesh axis runs over, the one named last changes fastest.
Arguments:
- tokens: bfloat16 [8, 1024, 1024], P('dp', 'seq'), may hold values from -6 to 6
- segments: int32 [8, 1024], P('dp'), may hold values from 0 to 6, as said below
- w_qkv: bfloat16 [1024, 3072], P('dp'), may hold values from -0.1875 to 0.1875
- w_attn_out: bfloat16 [1024, 1024], P('dp'), may hold values from -0.1875 to 0.1875
- w_in: bfloat16 [1024, 8192], P('dp'), may hold values from -0.1875 to 0.1875
- w_down: bfloat16 [4096, 1024], P('dp'), may hold values from -0.09375 to 0.09375
- s_qk: float32 [1024], replicated, may hold values from 1 to 1.8
- s_u: float32 [4096], replicated, may hold values from 0.5 to 2
- s_v: float32 [4096], replicated, may hold values from 0.5 to 2
- alpha_attn: float32 [1024], replicated, may hold values from 0.05 to 0.4
- alpha_mlp: float32 [1024], replicated, may hold values from 0.05 to 0.4
- cotangent: bfloat16 [8, 1024, 1024], P('dp', 'seq'), may hold values from -6 to 6
Outputs:
- output: bfloat16 [8, 1024, 1024], P('dp', 'seq')
- grad_tokens: float32 [8, 1024, 1024], P('dp', 'seq')
- grad_w_qkv: float32 [1024, 3072], P(('dp', 'seq'))
- grad_w_attn_out: float32 [1024, 1024], P(('dp', 'seq'))
- grad_w_in: float32 [1024, 8192], P(('dp', 'seq'))
- grad_w_down: float32 [4096, 1024], P(('dp', 'seq'))
- grad_s_qk: float32 [1024], P(('dp', 'seq'))
- grad_s_u: float32 [4096], P(('dp', 'seq'))
- grad_s_v: float32 [4096], P(('dp', 'seq'))
- grad_alpha_attn: float32 [1024], P(('dp', 'seq'))
- grad_alpha_mlp: float32 [1024], P(('dp', 'seq'))
The draws below stay inside these ranges and needn't reach their ends.
Inputs may be any that keep to these rules, and one draw needn't show every extreme that they name: `segments`: in each sequence ids count documents from 1 at the first token and rise by one at each new document; documents hold 200 to 2000 tokens except where a sequence's end cuts one; each sequence ends in 1 to 199 padding tokens of id 0; in one sequence of each draw every whole document holds exactly 200 tokens and one padding token ends it.
All inputs are finite; a program needn't handle non-finite values.
Results may differ from the reference program's by a relative error of at most 0.019.
Values may be sent and summed in bfloat16 or wider, within the bound.
A program may use at most 192 MiB of HBM per device.

```python
import math
import jax
import jax.numpy as jnp
from jax import lax

D = 1024
HEADS = 16
HD = 64
FF = 4096
DOC_MIN = 200
DOC_MAX = 2000
SEQS = 8
LEN = 1024


def draw_segments(key, part):
    key_lengths = jax.random.fold_in(key, 11)
    key_padding = jax.random.fold_in(key, 12)
    key_dense = jax.random.fold_in(key, 13)
    doc_count = LEN // DOC_MIN + 1
    dense_row = jax.random.randint(key_dense, (), 0, SEQS).astype(jnp.int32)
    is_dense = jnp.arange(SEQS, dtype=jnp.int32) == dense_row
    doc_sizes = jax.random.randint(key_lengths, (SEQS, doc_count), DOC_MIN, DOC_MAX + 1).astype(jnp.int32)
    doc_sizes = jnp.where(is_dense[:, None], DOC_MIN, doc_sizes).astype(jnp.int32)
    doc_ends = jnp.cumsum(doc_sizes, axis=1)
    places = jnp.arange(LEN, dtype=jnp.int32)
    doc_ids = 1 + jnp.sum((doc_ends[:, None, :] <= places[None, :, None]).astype(jnp.int32), axis=-1)
    padding = jax.random.randint(key_padding, (SEQS, 1), 1, DOC_MIN).astype(jnp.int32)
    padding = jnp.where(is_dense[:, None], 1, padding).astype(jnp.int32)
    return jnp.where(places[None, :] >= LEN - padding, 0, doc_ids).astype(jnp.int32)


def block_levels(stream_key, dims, split, least, top_value):
    def one(axis_at, shards_of):
        heights = jax.random.uniform(jax.random.fold_in(jax.random.fold_in(stream_key, 6), axis_at), (shards_of,), jnp.float32, least / len(split), top_value / len(split))
        return jnp.repeat(jnp.exp(heights), dims[axis_at] // shards_of).reshape((-1,) + (1,) * (len(dims) - axis_at - 1))

    gain = one(*split[0])
    for cut in split[1:]:
        gain = gain * one(*cut)
    return gain


def gaussian(rng, extent, width, most, shards=(), kind=jnp.bfloat16):
    array = jax.random.normal(rng, extent, jnp.float32) * width
    if len(shards) > 0:
        array = block_levels(rng, extent, shards, -0.22, 0.18) * array
    return jnp.clip(array, min=-most, max=most).astype(kind)


def setup_inputs(seed: int = 0) -> dict:
    arg_keys = jax.random.split(jax.random.key(seed), 13)
    return {
        "tokens": gaussian(arg_keys[0], (SEQS, LEN, D), 1.0, 6.0, ((0, 8), (1, 4))),
        "segments": draw_segments(jax.random.fold_in(arg_keys[12], 71), 0),
        "w_qkv": gaussian(arg_keys[2], (D, 3 * D), D ** -0.5, 0.1875, ((0, 8),)),
        "w_attn_out": gaussian(arg_keys[3], (D, D), D ** -0.5, 0.1875, ((0, 8),)),
        "w_in": gaussian(arg_keys[4], (D, 2 * FF), D ** -0.5, 0.1875, ((0, 8),)),
        "w_down": gaussian(arg_keys[5], (FF, D), FF ** -0.5, 0.09375, ((0, 8),)),
        "s_qk": jnp.clip(jnp.exp(jax.random.uniform(arg_keys[6], (D,), jnp.float32, math.log(1.0), math.log(1.8))), 1.0, 1.8),
        "s_u": jnp.clip(jnp.exp(jax.random.uniform(arg_keys[7], (FF,), jnp.float32, math.log(0.5), math.log(2.0))), 0.5, 2.0),
        "s_v": jnp.clip(jnp.exp(jax.random.uniform(arg_keys[8], (FF,), jnp.float32, math.log(0.5), math.log(2.0))), 0.5, 2.0),
        "alpha_attn": jnp.clip(jnp.exp(jax.random.uniform(arg_keys[9], (D,), jnp.float32, math.log(0.05), math.log(0.4))), 0.05, 0.4),
        "alpha_mlp": jnp.clip(jnp.exp(jax.random.uniform(arg_keys[10], (D,), jnp.float32, math.log(0.05), math.log(0.4))), 0.05, 0.4),
        "cotangent": gaussian(arg_keys[11], (SEQS, LEN, D), 1.0, 6.0, ((0, 8), (1, 4))),
    }


@jax.custom_vjp
def low(v):
    return lax.optimization_barrier(v.astype(jnp.bfloat16)).astype(jnp.float32)

@jax.custom_vjp
def low_back(v):
    return v

def low_keep(v):
    return (low(v), None)

def low_pass(kept, grad):
    return (grad,)

def back_keep(v):
    return (v, None)

def back_low(kept, grad):
    return (low(grad),)
low.defvjp(low_keep, low_pass)
low_back.defvjp(back_keep, back_low)
EPS = 1e-06
ROPE_BASE = 10000.0
MASKED_SCORE = -1e+30
PRECISE = lax.Precision.HIGHEST

def product(left_arr, right_arr):
    return jnp.dot(left_arr, right_arr, precision=PRECISE, preferred_element_type=jnp.float32)

def rms_unit(values):
    return values * lax.rsqrt(lax.optimization_barrier(jnp.mean(values * values, axis=-1, keepdims=True)) + EPS)

def doc_positions(seg_row):
    length = seg_row.shape[0]
    places = jnp.arange(length, dtype=jnp.int32)
    is_start = jnp.concatenate([jnp.ones((1,), dtype=bool), seg_row[1:] != seg_row[:-1]])
    starts = lax.cummax(jnp.where(is_start, places, 0).astype(jnp.int32), axis=0)
    return (places - starts).astype(jnp.float32)

def rope_tables(positions, head_dim):
    half_dim = head_dim // 2
    inverse_freq = ROPE_BASE ** (-(jnp.arange(half_dim, dtype=jnp.float32) * 2.0 / head_dim))
    angles = positions[:, None] * inverse_freq[None, :]
    return (jnp.cos(angles)[:, None, :], jnp.sin(angles)[:, None, :])

def rotate(values, cosine, sine_tab):
    half_dim = values.shape[-1] // 2
    low_half = values[..., :half_dim]
    high_half = values[..., half_dim:]
    return jnp.concatenate([low_half * cosine - high_half * sine_tab, high_half * cosine + low_half * sine_tab], axis=-1)

def allowed(seg_row, block_start, block_len):
    query_idx = block_start + jnp.arange(block_len, dtype=jnp.int32)
    key_idx = jnp.arange(seg_row.shape[0], dtype=jnp.int32)
    seg_query = lax.dynamic_slice_in_dim(seg_row, block_start, block_len)
    same_doc = seg_query[:, None] == seg_row[None, :]
    causal = key_idx[None, :] <= query_idx[:, None]
    not_padding = (seg_query[:, None] != 0) | (key_idx[None, :] == query_idx[:, None])
    return causal & same_doc & not_padding

def attention(query_n, key_n, value_f, seg_row):
    length, heads_all, head_dim = query_n.shape
    block_len = min(512, length)
    block_count = length // block_len
    score_scale = 1.0 / math.sqrt(head_dim)
    query_blocks = query_n.reshape(block_count, block_len, heads_all, head_dim)
    starts = jnp.arange(block_count, dtype=jnp.int32) * block_len

    def one_block(block_in):
        query_part, block_start = block_in
        scores = jnp.einsum('qhd,khd->hqk', query_part, key_n, precision=PRECISE) * score_scale
        scores = low_back(scores)
        mask_ok = allowed(seg_row, block_start, block_len)
        attn_probs = jax.nn.softmax(jnp.where(mask_ok[None], scores, MASKED_SCORE), axis=-1)
        attn_probs = low(attn_probs)
        return jnp.einsum('hqk,khd->qhd', attn_probs, value_f, precision=PRECISE)
    attn_mixed = lax.map(jax.checkpoint(one_block), (query_blocks, starts))
    return attn_mixed.reshape(length, heads_all * head_dim)

def one_sequence(params, seq_in):
    w_qkv, w_attn_out, w_in, w_down, s_qk, s_u, s_v, alpha_attn, alpha_mlp = params
    inputs, seg_row = seq_in
    length = inputs.shape[0]
    projected = low_back(low(product(inputs, w_qkv))).reshape(length, 3, HEADS, HD)
    cosine, sine_tab = rope_tables(doc_positions(seg_row), HD)
    head_gain = s_qk.reshape(HEADS, HD)
    query_n = low(rms_unit(rotate(projected[:, 0], cosine, sine_tab)) * head_gain)
    key_n = low(rms_unit(rotate(projected[:, 1], cosine, sine_tab)) * head_gain)
    attn_mixed = low_back(low(attention(query_n, key_n, projected[:, 2], seg_row)))
    attn_unit = rms_unit(low_back(product(attn_mixed, w_attn_out)))
    hidden = rms_unit(inputs + alpha_attn * (attn_unit - inputs))
    up_gate = low_back(product(low(hidden), w_in))
    ff_width = s_u.shape[0]
    inner_act = low(jax.nn.silu(s_v * up_gate[:, ff_width:]) * (s_u * up_gate[:, :ff_width]))
    mlp_unit = rms_unit(low_back(product(inner_act, w_down)))
    return rms_unit(hidden + alpha_mlp * (mlp_unit - hidden))

def reference(tokens, segments, w_qkv, w_attn_out, w_in, w_down, s_qk, s_u, s_v, alpha_attn, alpha_mlp, cotangent):
    floats = tuple((arr.astype(jnp.float32) for arr in (tokens, w_qkv, w_attn_out, w_in, w_down, s_qk, s_u, s_v, alpha_attn, alpha_mlp)))

    def forward(inputs, *params):

        def per_sequence(seq_in):
            return one_sequence(params, seq_in)
        return lax.map(jax.checkpoint(per_sequence), (inputs, segments))
    result, pullback = jax.vjp(forward, *floats)
    gradients = pullback(cotangent.astype(jnp.float32))
    return (result.astype(jnp.bfloat16), gradients[0], gradients[1], gradients[2], gradients[3], gradients[4], gradients[5], gradients[6], gradients[7], gradients[8], gradients[9])
```

```python
import math

import jax
import jax.numpy as jnp
from jax import lax
from jax.sharding import PartitionSpec as P

HEADS = 16
HD = 64


EPS = 1e-06
ROPE_BASE = 10000.0
MASKED_SCORE = -1e30


def as_sent(array):

    def short(part):
        return part.astype(jnp.bfloat16) if part.dtype == jnp.float32 else part

    return jax.tree.map(short, array)


def rms_norm(values):
    inverse = lax.rsqrt(jnp.mean(values * values, axis=-1, keepdims=True) + EPS)
    return (values * inverse, inverse)


def rms_back(grad_in, normed, inverse):
    return inverse * (grad_in - normed * jnp.mean(grad_in * normed, axis=-1, keepdims=True))


def contract_rows(left_arr, right_arr):
    return lax.dot_general(
        left_arr, right_arr, (((0,), (0,)), ((), ())), preferred_element_type=jnp.float32
    )


def contract_cols(left_arr, right_arr):
    return lax.dot_general(
        left_arr, right_arr, (((1,), (1,)), ((), ())), preferred_element_type=jnp.float32
    )


def doc_positions(seg_row):
    length = seg_row.shape[0]
    places = jnp.arange(length, dtype=jnp.int32)
    is_start = jnp.concatenate([jnp.ones((1,), dtype=bool), seg_row[1:] != seg_row[:-1]])
    starts = lax.cummax(jnp.where(is_start, places, 0), axis=0)
    return (places - starts).astype(jnp.float32)


def rope_tables(positions, head_dim):
    half_dim = head_dim // 2
    inverse_freq = ROPE_BASE ** (-(jnp.arange(half_dim, dtype=jnp.float32) * 2.0 / head_dim))
    angles = positions[:, None] * inverse_freq[None, :]
    return (jnp.cos(angles)[:, None, :], jnp.sin(angles)[:, None, :])


def rotate(values, cosine, sine_tab):
    half_dim = values.shape[-1] // 2
    low_half = values[..., :half_dim]
    high_half = values[..., half_dim:]
    return jnp.concatenate(
        [low_half * cosine - high_half * sine_tab, high_half * cosine + low_half * sine_tab],
        axis=-1,
    )


def head_prep(head_raw, cosine, sine_tab, head_gain):
    rotated = rotate(head_raw.astype(jnp.float32), cosine, sine_tab)
    head_unit, inverse = rms_norm(rotated)
    return (head_unit, inverse, (head_unit * head_gain).astype(jnp.bfloat16))


def head_back(grad_n, head_unit, inverse, head_gain, cosine, sine_tab):
    grad_rot = rms_back(grad_n * head_gain, head_unit, inverse)
    return rotate(grad_rot, cosine, -sine_tab)


def allowed(seg_row, block_start, block_len):
    query_idx = block_start + jnp.arange(block_len, dtype=jnp.int32)
    key_idx = jnp.arange(seg_row.shape[0], dtype=jnp.int32)
    seg_query = lax.dynamic_slice_in_dim(seg_row, block_start, block_len)
    same_doc = seg_query[:, None] == seg_row[None, :]
    causal = key_idx[None, :] <= query_idx[:, None]
    not_padding = (seg_query[:, None] != 0) | (key_idx[None, :] == query_idx[:, None])
    return causal & same_doc & not_padding


def attend_forward(query_n, key_n, value_b, seg_row, score_scale):
    length, groups, head_dim = query_n.shape
    block_len = min(512, length)
    block_count = length // block_len
    query_blocks = query_n.reshape(block_count, block_len, groups, head_dim)
    starts = jnp.arange(block_count, dtype=jnp.int32) * block_len

    def one_block(block_in):
        query_part, block_start = block_in
        scores = (
            jnp.einsum("qhd,khd->hqk", query_part, key_n, preferred_element_type=jnp.float32)
            * score_scale
        )
        mask_ok = allowed(seg_row, block_start, block_len)
        scores = jnp.where(mask_ok[None], scores, MASKED_SCORE)
        row_max = jnp.max(scores, axis=-1, keepdims=True)
        weights_exp = jnp.exp(scores - row_max)
        row_total = jnp.sum(weights_exp, axis=-1, keepdims=True)
        attn_probs = (weights_exp / row_total).astype(jnp.bfloat16)
        attn_part = jnp.einsum(
            "hqk,khd->qhd", attn_probs, value_b, preferred_element_type=jnp.float32
        )
        return (attn_part.astype(jnp.bfloat16), (row_max + jnp.log(row_total))[..., 0])

    attn_mixed, log_sums = lax.map(one_block, (query_blocks, starts))
    return (attn_mixed.reshape(length, groups * head_dim), log_sums)


def attend_backward(query_n, key_n, value_b, grad_attn, log_sums, seg_row, score_scale):
    length, groups, head_dim = query_n.shape
    block_len = min(512, length)
    block_count = length // block_len
    query_blocks = query_n.reshape(block_count, block_len, groups, head_dim)
    grad_blocks = grad_attn.reshape(block_count, block_len, groups, head_dim)
    starts = jnp.arange(block_count, dtype=jnp.int32) * block_len

    def one_block(accums, block_in):
        key_acc, value_acc = accums
        query_part, grad_part, lse_part, block_start = block_in
        scores = (
            jnp.einsum("qhd,khd->hqk", query_part, key_n, preferred_element_type=jnp.float32)
            * score_scale
        )
        mask_ok = allowed(seg_row, block_start, block_len)
        attn_probs = jnp.where(mask_ok[None], jnp.exp(scores - lse_part[..., None]), 0.0)
        grad_probs = jnp.einsum(
            "qhd,khd->hqk", grad_part, value_b, preferred_element_type=jnp.float32
        )
        delta_row = jnp.sum(grad_probs * attn_probs, axis=-1, keepdims=True)
        grad_scores = (attn_probs * (grad_probs - delta_row)).astype(jnp.bfloat16)
        grad_query = (
            jnp.einsum("hqk,khd->qhd", grad_scores, key_n, preferred_element_type=jnp.float32)
            * score_scale
        )
        key_acc = (
            key_acc
            + jnp.einsum(
                "hqk,qhd->khd", grad_scores, query_part, preferred_element_type=jnp.float32
            )
            * score_scale
        )
        value_acc = value_acc + jnp.einsum(
            "hqk,qhd->khd",
            attn_probs.astype(jnp.bfloat16),
            grad_part,
            preferred_element_type=jnp.float32,
        )
        return ((key_acc, value_acc), grad_query)

    zeros_init = jnp.zeros((length, groups, head_dim), jnp.float32)
    (grad_key, grad_value), grad_query = lax.scan(
        one_block, (zeros_init, zeros_init), (query_blocks, grad_blocks, log_sums, starts)
    )
    return (grad_query.reshape(length, groups, head_dim), grad_key, grad_value)


def body(
    tokens,
    segments,
    w_qkv,
    w_attn_out,
    w_in,
    w_down,
    s_qk,
    s_u,
    s_v,
    alpha_attn,
    alpha_mlp,
    cotangent,
):
    model_width = tokens.shape[-1]
    inputs_b = tokens.reshape(-1, model_width)
    inputs_f = inputs_b.astype(jnp.float32)
    seg_row = segments.reshape(-1)
    seq_count = lax.axis_size("seq")
    dp_count = lax.axis_size("dp")
    head_group = HEADS // seq_count
    group_width = head_group * HD
    offset = lax.axis_index("seq") * group_width
    head_gain = lax.dynamic_slice_in_dim(s_qk, offset, group_width).reshape(head_group, HD)
    score_scale = 1.0 / math.sqrt(HD)
    full_qkv, full_out, full_in, full_down = (
        lax.all_gather(w_qkv, "dp", axis=0, tiled=True),
        lax.all_gather(w_attn_out, "dp", axis=0, tiled=True),
        lax.all_gather(w_in, "dp", axis=0, tiled=True),
        lax.all_gather(w_down, "dp", axis=0, tiled=True),
    )
    projected = jnp.dot(inputs_b, full_qkv, preferred_element_type=jnp.float32).astype(jnp.bfloat16)
    by_heads = lax.all_to_all(
        projected.reshape(-1, 3, model_width), "seq", split_axis=2, concat_axis=0, tiled=True
    )
    length = by_heads.shape[0]
    cosine, sine_tab = rope_tables(doc_positions(seg_row), HD)
    query_unit, query_inv, query_n = head_prep(
        by_heads[:, 0].reshape(length, head_group, HD), cosine, sine_tab, head_gain
    )
    key_unit, key_inv, key_n = head_prep(
        by_heads[:, 1].reshape(length, head_group, HD), cosine, sine_tab, head_gain
    )
    value_b = by_heads[:, 2].reshape(length, head_group, HD)
    attn_mixed, log_sums = attend_forward(query_n, key_n, value_b, seg_row, score_scale)
    attn_pieces = lax.all_to_all(attn_mixed, "seq", split_axis=0, concat_axis=1, tiled=True)
    attn_proj = jnp.dot(attn_pieces, full_out, preferred_element_type=jnp.float32)
    attn_unit, attn_inv = rms_norm(attn_proj)
    hidden, hidden_inv = rms_norm(inputs_f + alpha_attn * (attn_unit - inputs_f))
    hidden_b = hidden.astype(jnp.bfloat16)
    up_gate = jnp.dot(hidden_b, full_in, preferred_element_type=jnp.float32)
    ff_width = s_u.shape[0]
    up_raw = up_gate[:, :ff_width]
    gate_raw = up_gate[:, ff_width:]
    up_val = s_u * up_raw
    gate_val = s_v * gate_raw
    gate_sig = jax.nn.sigmoid(gate_val)
    silu_gate = gate_val * gate_sig
    inner_act = (silu_gate * up_val).astype(jnp.bfloat16)
    down_proj = jnp.dot(inner_act, full_down, preferred_element_type=jnp.float32)
    mlp_unit, mlp_inv = rms_norm(down_proj)
    result, result_inv = rms_norm(hidden + alpha_mlp * (mlp_unit - hidden))
    output = result.astype(jnp.bfloat16).reshape(tokens.shape)
    grad_res = cotangent.reshape(-1, model_width).astype(jnp.float32)
    grad_two = rms_back(grad_res, result, result_inv)
    grad_alpha_mlp = jnp.sum(grad_two * (mlp_unit - hidden), axis=0)
    grad_down_proj = rms_back(alpha_mlp * grad_two, mlp_unit, mlp_inv).astype(jnp.bfloat16)
    grad_w_down = contract_rows(inner_act, grad_down_proj)
    grad_inner = contract_cols(grad_down_proj, full_down)
    grad_up_val = grad_inner * silu_gate
    grad_gate_val = grad_inner * up_val * gate_sig * (1.0 + gate_val * (1.0 - gate_sig))
    grad_s_u = jnp.sum(grad_up_val * up_raw, axis=0)
    grad_s_v = jnp.sum(grad_gate_val * gate_raw, axis=0)
    grad_up_gate = jnp.concatenate([grad_up_val * s_u, grad_gate_val * s_v], axis=1).astype(
        jnp.bfloat16
    )
    grad_w_in = contract_rows(hidden_b, grad_up_gate)
    grad_hidden = (1.0 - alpha_mlp) * grad_two + contract_cols(grad_up_gate, full_in)
    grad_one = rms_back(grad_hidden, hidden, hidden_inv)
    grad_alpha_attn = jnp.sum(grad_one * (attn_unit - inputs_f), axis=0)
    grad_attn_proj = rms_back(alpha_attn * grad_one, attn_unit, attn_inv).astype(jnp.bfloat16)
    grad_w_attn_out = contract_rows(attn_pieces, grad_attn_proj)
    grad_pieces = contract_cols(grad_attn_proj, full_out).astype(jnp.bfloat16)
    grad_heads = lax.all_to_all(
        grad_pieces, "seq", split_axis=1, concat_axis=0, tiled=True
    ).reshape(length, head_group, HD)
    grad_query_n, grad_key_n, grad_value = attend_backward(
        query_n, key_n, value_b, grad_heads, log_sums, seg_row, score_scale
    )
    grad_head_gain = jnp.sum(grad_query_n * query_unit + grad_key_n * key_unit, axis=0)
    grad_query = head_back(grad_query_n, query_unit, query_inv, head_gain, cosine, sine_tab)
    grad_key = head_back(grad_key_n, key_unit, key_inv, head_gain, cosine, sine_tab)
    grad_stack = (
        jnp.stack([grad_query, grad_key, grad_value], axis=1)
        .reshape(length, 3, group_width)
        .astype(jnp.bfloat16)
    )
    grad_qkv = lax.all_to_all(grad_stack, "seq", split_axis=0, concat_axis=2, tiled=True).reshape(
        -1, 3 * model_width
    )
    grad_w_qkv = contract_rows(inputs_b, grad_qkv)
    grad_inputs = (1.0 - alpha_attn) * grad_one + contract_cols(grad_qkv, full_qkv)
    grad_s_qk = lax.dynamic_update_slice_in_dim(
        jnp.zeros((model_width,), jnp.float32), grad_head_gain.reshape(-1), offset, 0
    )
    big_terms = (grad_w_qkv, grad_w_attn_out, grad_w_in, grad_w_down)
    across = tuple(
        (
            lax.psum_scatter(term, "dp", scatter_dimension=0, tiled=True)
            for term in as_sent(big_terms)
        )
    )
    big_shards = tuple(
        (
            lax.psum_scatter(term, "seq", scatter_dimension=0, tiled=True).astype(jnp.float32)
            for term in across
        )
    )
    small_terms = (grad_s_qk, grad_s_u, grad_s_v, grad_alpha_attn, grad_alpha_mlp)
    packed = jnp.concatenate(
        [term.reshape(dp_count * seq_count, -1) for term in small_terms], axis=1
    )
    packed = lax.psum_scatter(packed, ("dp", "seq"), scatter_dimension=0, tiled=True).reshape(-1)
    small_shards = []
    place = 0
    for term in small_terms:
        width = term.shape[0] // (dp_count * seq_count)
        small_shards.append(packed[place : place + width])
        place += width
    shards = big_shards + tuple(small_shards)
    return (output, grad_inputs.reshape(tokens.shape)) + tuple(shards)


def solution(mesh):
    placed = (
        P("dp", "seq", None),
        P("dp", None),
        P("dp", None),
        P("dp", None),
        P("dp", None),
        P("dp", None),
        P(),
        P(),
        P(),
        P(),
        P(),
        P("dp", "seq", None),
    )
    return jax.shard_map(
        body,
        mesh=mesh,
        in_specs=placed,
        out_specs=(
            P("dp", "seq", None),
            P("dp", "seq", None),
            P(("dp", "seq"), None),
            P(("dp", "seq"), None),
            P(("dp", "seq"), None),
            P(("dp", "seq"), None),
            P(("dp", "seq")),
            P(("dp", "seq")),
            P(("dp", "seq")),
            P(("dp", "seq")),
            P(("dp", "seq")),
        ),
        check_vma=False,
    )
```

```python
import functools
import math

import jax
import jax.numpy as jnp
from jax import lax
from jax.experimental import pallas as pl
from jax.experimental.pallas import tpu as pltpu
from jax.sharding import PartitionSpec as P

MESH_ID = pl.DeviceIdType.MESH
TEAM = 4

HEADS = 16
HD = 64


EPS = 1e-06
ROPE_BASE = 10000.0
MASKED_SCORE = -1e30


def rms_norm(values):
    inverse = lax.rsqrt(jnp.mean(values * values, axis=-1, keepdims=True) + EPS)
    return (values * inverse, inverse)


def rms_back(grad_in, normed, inverse):
    return inverse * (grad_in - normed * jnp.mean(grad_in * normed, axis=-1, keepdims=True))


def contract_rows(left_arr, right_arr):
    return lax.dot_general(
        left_arr, right_arr, (((0,), (0,)), ((), ())), preferred_element_type=jnp.float32
    )


def contract_cols(left_arr, right_arr):
    return lax.dot_general(
        left_arr, right_arr, (((1,), (1,)), ((), ())), preferred_element_type=jnp.float32
    )


def doc_positions(seg_row):
    length = seg_row.shape[0]
    places = jnp.arange(length, dtype=jnp.int32)
    is_start = jnp.concatenate([jnp.ones((1,), dtype=bool), seg_row[1:] != seg_row[:-1]])
    starts = lax.cummax(jnp.where(is_start, places, 0), axis=0)
    return (places - starts).astype(jnp.float32)


def rope_tables(positions, head_dim):
    half_dim = head_dim // 2
    inverse_freq = ROPE_BASE ** (-(jnp.arange(half_dim, dtype=jnp.float32) * 2.0 / head_dim))
    angles = positions[:, None] * inverse_freq[None, :]
    return (jnp.cos(angles)[:, None, :], jnp.sin(angles)[:, None, :])


def rotate(values, cosine, sine_tab):
    half_dim = values.shape[-1] // 2
    low_half = values[..., :half_dim]
    high_half = values[..., half_dim:]
    return jnp.concatenate(
        [low_half * cosine - high_half * sine_tab, high_half * cosine + low_half * sine_tab],
        axis=-1,
    )


def head_prep(head_raw, cosine, sine_tab, head_gain):
    rotated = rotate(head_raw.astype(jnp.float32), cosine, sine_tab)
    head_unit, inverse = rms_norm(rotated)
    return (head_unit, inverse, (head_unit * head_gain).astype(jnp.bfloat16))


def head_back(grad_n, head_unit, inverse, head_gain, cosine, sine_tab):
    grad_rot = rms_back(grad_n * head_gain, head_unit, inverse)
    return rotate(grad_rot, cosine, -sine_tab)


def allowed(seg_row, block_start, block_len):
    query_idx = block_start + jnp.arange(block_len, dtype=jnp.int32)
    key_idx = jnp.arange(seg_row.shape[0], dtype=jnp.int32)
    seg_query = lax.dynamic_slice_in_dim(seg_row, block_start, block_len)
    same_doc = seg_query[:, None] == seg_row[None, :]
    causal = key_idx[None, :] <= query_idx[:, None]
    not_padding = (seg_query[:, None] != 0) | (key_idx[None, :] == query_idx[:, None])
    return causal & same_doc & not_padding


def attend_forward(query_n, key_n, value_b, seg_row, score_scale):
    length, groups, head_dim = query_n.shape
    block_len = min(512, length)
    block_count = length // block_len
    query_blocks = query_n.reshape(block_count, block_len, groups, head_dim)
    starts = jnp.arange(block_count, dtype=jnp.int32) * block_len

    def one_block(block_in):
        query_part, block_start = block_in
        scores = (
            jnp.einsum("qhd,khd->hqk", query_part, key_n, preferred_element_type=jnp.float32)
            * score_scale
        )
        mask_ok = allowed(seg_row, block_start, block_len)
        scores = jnp.where(mask_ok[None], scores, MASKED_SCORE)
        row_max = jnp.max(scores, axis=-1, keepdims=True)
        weights_exp = jnp.exp(scores - row_max)
        row_total = jnp.sum(weights_exp, axis=-1, keepdims=True)
        attn_probs = (weights_exp / row_total).astype(jnp.bfloat16)
        attn_part = jnp.einsum(
            "hqk,khd->qhd", attn_probs, value_b, preferred_element_type=jnp.float32
        )
        return (attn_part.astype(jnp.bfloat16), (row_max + jnp.log(row_total))[..., 0])

    attn_mixed, log_sums = lax.map(one_block, (query_blocks, starts))
    return (attn_mixed.reshape(length, groups * head_dim), log_sums)


def attend_backward(query_n, key_n, value_b, grad_attn, log_sums, seg_row, score_scale):
    length, groups, head_dim = query_n.shape
    block_len = min(512, length)
    block_count = length // block_len
    query_blocks = query_n.reshape(block_count, block_len, groups, head_dim)
    grad_blocks = grad_attn.reshape(block_count, block_len, groups, head_dim)
    starts = jnp.arange(block_count, dtype=jnp.int32) * block_len

    def one_block(accums, block_in):
        key_acc, value_acc = accums
        query_part, grad_part, lse_part, block_start = block_in
        scores = (
            jnp.einsum("qhd,khd->hqk", query_part, key_n, preferred_element_type=jnp.float32)
            * score_scale
        )
        mask_ok = allowed(seg_row, block_start, block_len)
        attn_probs = jnp.where(mask_ok[None], jnp.exp(scores - lse_part[..., None]), 0.0)
        grad_probs = jnp.einsum(
            "qhd,khd->hqk", grad_part, value_b, preferred_element_type=jnp.float32
        )
        delta_row = jnp.sum(grad_probs * attn_probs, axis=-1, keepdims=True)
        grad_scores = (attn_probs * (grad_probs - delta_row)).astype(jnp.bfloat16)
        grad_query = (
            jnp.einsum("hqk,khd->qhd", grad_scores, key_n, preferred_element_type=jnp.float32)
            * score_scale
        )
        key_acc = (
            key_acc
            + jnp.einsum(
                "hqk,qhd->khd", grad_scores, query_part, preferred_element_type=jnp.float32
            )
            * score_scale
        )
        value_acc = value_acc + jnp.einsum(
            "hqk,qhd->khd",
            attn_probs.astype(jnp.bfloat16),
            grad_part,
            preferred_element_type=jnp.float32,
        )
        return ((key_acc, value_acc), grad_query)

    zeros_init = jnp.zeros((length, groups, head_dim), jnp.float32)
    (grad_key, grad_value), grad_query = lax.scan(
        one_block, (zeros_init, zeros_init), (query_blocks, grad_blocks, log_sums, starts)
    )
    return (grad_query.reshape(length, groups, head_dim), grad_key, grad_value)


def greet(peers):
    barrier = pltpu.get_barrier_semaphore()
    for peer in peers:
        pl.semaphore_signal(barrier, inc=1, device_id=peer, device_id_type=MESH_ID)
    pl.semaphore_wait(barrier, len(peers))


def flip(place, bit):
    return place + bit - 2 * bit * lax.rem(place // bit, 2)


def seq_gather_kernel(count, own_ref, out_ref, send_sem, recv_sem, local_sem):
    rows = own_ref.shape[0]
    mine = lax.axis_index("seq")
    peers = [lax.rem(mine + step, count) for step in range(1, count)]
    greet([{"seq": peer} for peer in peers])
    spot = pl.ds(pl.multiple_of(mine * rows, rows), rows)
    copies = []
    for slot, peer in enumerate(peers):
        copies.append(
            pltpu.make_async_remote_copy(
                src_ref=own_ref,
                dst_ref=out_ref.at[spot],
                send_sem=send_sem.at[slot],
                recv_sem=recv_sem.at[slot],
                device_id={"seq": peer},
                device_id_type=MESH_ID,
            )
        )
    for copy in copies:
        copy.start()
    local = pltpu.make_async_copy(own_ref, out_ref.at[spot], local_sem)
    local.start()
    local.wait()
    for copy in copies:
        copy.wait()


def seq_gather(own):
    count = lax.axis_size("seq")
    rows, width = own.shape
    return pl.pallas_call(
        functools.partial(seq_gather_kernel, count),
        out_shape=jax.ShapeDtypeStruct((count * rows, width), own.dtype),
        in_specs=[pl.BlockSpec(memory_space=pl.ANY)],
        out_specs=pl.BlockSpec(memory_space=pl.ANY),
        scratch_shapes=[
            pltpu.SemaphoreType.DMA((count - 1,)),
            pltpu.SemaphoreType.DMA((count - 1,)),
            pltpu.SemaphoreType.DMA,
        ],
        cost_estimate=pl.CostEstimate(
            flops=0, bytes_accessed=100 * count * rows * width, transcendentals=0
        ),
        compiler_params=pltpu.CompilerParams(collective_id=0, has_side_effects=True),
    )(own)


PIECES = 4


def team_gather_kernel(own_ref, out_ref, send_sem, recv_sem, local_sem):
    rows = own_ref.shape[0]
    piece = rows // PIECES
    place = lax.axis_index("dp")
    far, near = flip(place, 2), flip(place, 1)
    rank, far_rank = lax.rem(place, TEAM), lax.rem(far, TEAM)
    greet([{"dp": far}, {"dp": near}])

    def spot(owner, index):
        return out_ref.at[pl.ds(pl.multiple_of(owner * rows + index * piece, piece), piece)]

    def push(source, owner, index, kind, peer):
        return pltpu.make_async_remote_copy(
            src_ref=source,
            dst_ref=spot(owner, index),
            send_sem=send_sem.at[kind, index],
            recv_sem=recv_sem.at[kind, index],
            device_id={"dp": peer},
            device_id_type=MESH_ID,
        )

    across = [push(own_ref.at[pl.ds(i * piece, piece)], rank, i, 0, far) for i in range(PIECES)]
    beside = [push(own_ref.at[pl.ds(i * piece, piece)], rank, i, 1, near) for i in range(PIECES)]
    for copy in across:
        copy.start()
    for copy in beside:
        copy.start()
    local = pltpu.make_async_copy(
        own_ref, out_ref.at[pl.ds(pl.multiple_of(rank * rows, rows), rows)], local_sem
    )
    local.start()
    passed = [push(spot(far_rank, i), far_rank, i, 2, near) for i in range(PIECES)]
    for i in range(PIECES):
        across[i].wait_recv()
        passed[i].start()
    local.wait()
    for copy in across:
        copy.wait_send()
    for copy in beside:
        copy.wait()
    for copy in passed:
        copy.wait()


def team_gather(own):
    rows, width = own.shape
    return pl.pallas_call(
        team_gather_kernel,
        out_shape=jax.ShapeDtypeStruct((TEAM * rows, width), own.dtype),
        in_specs=[pl.BlockSpec(memory_space=pl.ANY)],
        out_specs=pl.BlockSpec(memory_space=pl.ANY),
        scratch_shapes=[
            pltpu.SemaphoreType.DMA((3, PIECES)),
            pltpu.SemaphoreType.DMA((3, PIECES)),
            pltpu.SemaphoreType.DMA,
        ],
        cost_estimate=pl.CostEstimate(
            flops=0, bytes_accessed=50 * TEAM * rows * width, transcendentals=0
        ),
        compiler_params=pltpu.CompilerParams(collective_id=1, has_side_effects=True),
    )(own)


def team_sum_kernel(part_ref, out_ref, near_buf, send_buf, far_buf, send_sem, recv_sem, far_send, far_recv):
    rows = out_ref.shape[0]
    piece = rows // PIECES
    place = lax.axis_index("dp")
    far, near = flip(place, 2), flip(place, 1)
    rank, far_rank = lax.rem(place, TEAM), lax.rem(far, TEAM)
    near_rank = lax.rem(near, TEAM)
    cross_rank = lax.rem(flip(near, 2), TEAM)
    greet([{"dp": far}, {"dp": near}])

    def to_near(owner, slot, index):
        return pltpu.make_async_remote_copy(
            src_ref=part_ref.at[owner, pl.ds(index * piece, piece)],
            dst_ref=near_buf.at[slot, pl.ds(index * piece, piece)],
            send_sem=send_sem.at[slot, index],
            recv_sem=recv_sem.at[slot, index],
            device_id={"dp": near},
            device_id_type=MESH_ID,
        )

    outward = [to_near(cross_rank, 0, i) for i in range(PIECES)]
    inward = [to_near(near_rank, 1, i) for i in range(PIECES)]
    for copy in outward + inward:
        copy.start()
    ships = []
    for i in range(PIECES):
        here = pl.ds(i * piece, piece)
        outward[i].wait_recv()
        send_buf[here] = (
            part_ref[far_rank, here].astype(jnp.float32) + near_buf[0, here].astype(jnp.float32)
        ).astype(send_buf.dtype)
        ships.append(
            pltpu.make_async_remote_copy(
                src_ref=send_buf.at[here],
                dst_ref=far_buf.at[here],
                send_sem=far_send.at[i],
                recv_sem=far_recv.at[i],
                device_id={"dp": far},
                device_id_type=MESH_ID,
            )
        )
        if i > 0:
            ships[i - 1].start()
    for i in range(PIECES):
        here = pl.ds(i * piece, piece)
        inward[i].wait_recv()
        out_ref[here] = part_ref[rank, here].astype(jnp.float32) + near_buf[1, here].astype(
            jnp.float32
        )
        if i == 0:
            ships[PIECES - 1].start()
    for i in range(PIECES):
        here = pl.ds(i * piece, piece)
        ships[i].wait_recv()
        out_ref[here] = out_ref[here] + far_buf[here].astype(jnp.float32)
    for copy in outward + inward + ships:
        copy.wait_send()


def team_sum(part):
    _, rows, width = part.shape
    return pl.pallas_call(
        team_sum_kernel,
        out_shape=jax.ShapeDtypeStruct((rows, width), jnp.float32),
        in_specs=[pl.BlockSpec(memory_space=pltpu.VMEM)],
        out_specs=pl.BlockSpec(memory_space=pltpu.VMEM),
        scratch_shapes=[
            pltpu.VMEM((2, rows, width), part.dtype),
            pltpu.VMEM((rows, width), part.dtype),
            pltpu.VMEM((rows, width), part.dtype),
            pltpu.SemaphoreType.DMA((2, PIECES)),
            pltpu.SemaphoreType.DMA((2, PIECES)),
            pltpu.SemaphoreType.DMA((PIECES,)),
            pltpu.SemaphoreType.DMA((PIECES,)),
        ],
        cost_estimate=pl.CostEstimate(
            flops=0, bytes_accessed=50 * TEAM * rows * width, transcendentals=0
        ),
        compiler_params=pltpu.CompilerParams(collective_id=2, has_side_effects=True),
    )(part)


def body(
    tokens,
    segments,
    w_qkv,
    w_attn_out,
    w_in,
    w_down,
    s_qk,
    s_u,
    s_v,
    alpha_attn,
    alpha_mlp,
    cotangent,
):
    model_width = tokens.shape[-1]
    inputs_b = tokens.reshape(-1, model_width)
    inputs_f = inputs_b.astype(jnp.float32)
    seg_row = segments.reshape(-1)
    length = seg_row.shape[0]
    local_rows = inputs_b.shape[0]
    seq_count = lax.axis_size("seq")
    dp_count = lax.axis_size("dp")
    head_group = HEADS // seq_count
    group_width = head_group * HD
    seq_rank = lax.axis_index("seq")
    team_rank = lax.rem(lax.axis_index("dp"), TEAM)
    offset = seq_rank * group_width
    head_gain = lax.dynamic_slice_in_dim(s_qk, offset, group_width).reshape(head_group, HD)
    score_scale = 1.0 / math.sqrt(HD)
    ff_width = s_u.shape[0]
    ff_part = ff_width // dp_count // TEAM
    ff_team = ff_width // TEAM
    in_rows = w_in.shape[0]

    head_cols = lax.dynamic_slice_in_dim(
        w_qkv.reshape(-1, 3, model_width), offset, group_width, axis=2
    ).reshape(-1, 3 * group_width)
    heads_qkv = lax.all_gather(head_cols, "dp", axis=0, tiled=True)
    full_out = lax.all_gather(w_attn_out, "dp", axis=0, tiled=True)
    in_parts = w_in.reshape(in_rows, 2 * dp_count, TEAM, ff_part).transpose(2, 0, 1, 3)
    ff_blocks = jnp.concatenate(
        [
            in_parts.reshape(TEAM, in_rows, 2 * ff_team),
            w_down.reshape(TEAM, ff_part, model_width),
        ],
        axis=2,
    )
    ff_blocks = jnp.concatenate([ff_blocks] * (dp_count // TEAM), axis=0)
    team_ff = lax.all_to_all(ff_blocks, "dp", 0, 0, tiled=True)
    team_in = team_ff[:, :, : 2 * ff_team].reshape(model_width, 2 * ff_team)
    team_down = team_ff[:, :, 2 * ff_team :].reshape(ff_team, model_width)

    def team_slice(scale):
        return lax.dynamic_index_in_dim(
            scale.reshape(dp_count, TEAM, ff_part), team_rank, 1, keepdims=False
        ).reshape(ff_team)

    s_u_team, s_v_team = team_slice(s_u), team_slice(s_v)

    seq_tokens = seq_gather(inputs_b)
    by_heads = (
        jnp.dot(seq_tokens, heads_qkv, preferred_element_type=jnp.float32)
        .astype(jnp.bfloat16)
        .reshape(length, 3, group_width)
    )
    cosine, sine_tab = rope_tables(doc_positions(seg_row), HD)
    query_unit, query_inv, query_n = head_prep(
        by_heads[:, 0].reshape(length, head_group, HD), cosine, sine_tab, head_gain
    )
    key_unit, key_inv, key_n = head_prep(
        by_heads[:, 1].reshape(length, head_group, HD), cosine, sine_tab, head_gain
    )
    value_b = by_heads[:, 2].reshape(length, head_group, HD)
    attn_mixed, log_sums = attend_forward(query_n, key_n, value_b, seg_row, score_scale)
    attn_pieces = lax.all_to_all(attn_mixed, "seq", split_axis=0, concat_axis=1, tiled=True)
    attn_proj = jnp.dot(attn_pieces, full_out, preferred_element_type=jnp.float32)
    attn_unit, attn_inv = rms_norm(attn_proj)
    hidden, hidden_inv = rms_norm(inputs_f + alpha_attn * (attn_unit - inputs_f))
    hidden_b = hidden.astype(jnp.bfloat16)

    team_hidden = team_gather(hidden_b)
    up_gate = jnp.dot(team_hidden, team_in, preferred_element_type=jnp.float32)
    up_raw = up_gate[:, :ff_team]
    gate_raw = up_gate[:, ff_team:]
    up_val = s_u_team * up_raw
    gate_val = s_v_team * gate_raw
    gate_sig = jax.nn.sigmoid(gate_val)
    silu_gate = gate_val * gate_sig
    inner_act = (silu_gate * up_val).astype(jnp.bfloat16)
    down_part = jnp.dot(inner_act, team_down, preferred_element_type=jnp.float32)
    down_proj = team_sum(down_part.astype(jnp.bfloat16).reshape(TEAM, local_rows, model_width))
    mlp_unit, mlp_inv = rms_norm(down_proj)
    result, result_inv = rms_norm(hidden + alpha_mlp * (mlp_unit - hidden))
    output = result.astype(jnp.bfloat16).reshape(tokens.shape)
    grad_res = cotangent.reshape(-1, model_width).astype(jnp.float32)
    grad_two = rms_back(grad_res, result, result_inv)
    grad_alpha_mlp = jnp.sum(grad_two * (mlp_unit - hidden), axis=0)
    grad_down_proj = rms_back(alpha_mlp * grad_two, mlp_unit, mlp_inv).astype(jnp.bfloat16)

    team_grad = team_gather(grad_down_proj)
    grad_inner = contract_cols(team_grad, team_down)
    grad_up_val = grad_inner * silu_gate
    grad_gate_val = grad_inner * up_val * gate_sig * (1.0 + gate_val * (1.0 - gate_sig))
    grad_s_u = jnp.sum(grad_up_val * up_raw, axis=0)
    grad_s_v = jnp.sum(grad_gate_val * gate_raw, axis=0)
    grad_up_gate = jnp.concatenate(
        [grad_up_val * s_u_team, grad_gate_val * s_v_team], axis=1
    ).astype(jnp.bfloat16)
    hidden_part = contract_cols(grad_up_gate, team_in)
    hidden_sum = team_sum(hidden_part.astype(jnp.bfloat16).reshape(TEAM, local_rows, model_width))
    grad_hidden = (1.0 - alpha_mlp) * grad_two + hidden_sum
    grad_w_ff = jnp.concatenate(
        [contract_rows(team_hidden, grad_up_gate), contract_rows(inner_act, team_grad)], axis=1
    ).astype(jnp.bfloat16)
    ff_terms = lax.all_to_all(
        grad_w_ff.reshape(dp_count, in_rows, 2 * ff_team + model_width), "dp", 0, 0, tiled=True
    )
    ff_sums = jnp.sum(
        ff_terms.reshape(dp_count // TEAM, TEAM, in_rows, -1).astype(jnp.float32), axis=0
    ).astype(jnp.bfloat16)
    in_sums = ff_sums[:, :, : 2 * ff_team].transpose(1, 0, 2).reshape(in_rows, 2 * ff_width)
    shard_w_in = lax.psum_scatter(in_sums, "seq", scatter_dimension=0, tiled=True)
    shard_w_in = (
        shard_w_in.reshape(-1, TEAM, 2 * dp_count, ff_part)
        .transpose(0, 2, 1, 3)
        .reshape(-1, 2 * ff_width)
        .astype(jnp.float32)
    )
    shard_w_down = lax.psum_scatter(
        ff_sums[:, :, 2 * ff_team :].reshape(TEAM * ff_part, model_width),
        "seq",
        scatter_dimension=0,
        tiled=True,
    ).astype(jnp.float32)

    grad_one = rms_back(grad_hidden, hidden, hidden_inv)
    grad_alpha_attn = jnp.sum(grad_one * (attn_unit - inputs_f), axis=0)
    grad_attn_proj = rms_back(alpha_attn * grad_one, attn_unit, attn_inv).astype(jnp.bfloat16)
    grad_pieces = contract_cols(grad_attn_proj, full_out).astype(jnp.bfloat16)
    grad_w_attn_out = contract_rows(attn_pieces, grad_attn_proj).astype(jnp.bfloat16)
    shard_w_attn_out = lax.psum_scatter(
        lax.psum_scatter(grad_w_attn_out, "dp", scatter_dimension=0, tiled=True),
        "seq",
        scatter_dimension=0,
        tiled=True,
    ).astype(jnp.float32)
    grad_heads = lax.all_to_all(
        grad_pieces, "seq", split_axis=1, concat_axis=0, tiled=True
    ).reshape(length, head_group, HD)
    grad_query_n, grad_key_n, grad_value = attend_backward(
        query_n, key_n, value_b, grad_heads, log_sums, seg_row, score_scale
    )
    grad_head_gain = jnp.sum(grad_query_n * query_unit + grad_key_n * key_unit, axis=0)
    grad_query = head_back(grad_query_n, query_unit, query_inv, head_gain, cosine, sine_tab)
    grad_key = head_back(grad_key_n, key_unit, key_inv, head_gain, cosine, sine_tab)
    grad_qkv = (
        jnp.stack([grad_query, grad_key, grad_value], axis=1)
        .reshape(length, 3 * group_width)
        .astype(jnp.bfloat16)
    )
    grad_w_qkv = contract_rows(seq_tokens, grad_qkv).astype(jnp.bfloat16)
    rows_w_qkv = lax.psum_scatter(grad_w_qkv, "dp", scatter_dimension=0, tiled=True)
    shard_w_qkv = lax.all_to_all(
        rows_w_qkv.reshape(seq_count, -1, 3 * group_width), "seq", 0, 0, tiled=True
    )
    shard_w_qkv = (
        shard_w_qkv.reshape(seq_count, -1, 3, group_width)
        .transpose(1, 2, 0, 3)
        .reshape(-1, 3 * model_width)
        .astype(jnp.float32)
    )
    tokens_part = contract_cols(grad_qkv, heads_qkv).astype(jnp.bfloat16)
    tokens_terms = lax.all_to_all(
        tokens_part.reshape(seq_count, local_rows, model_width), "seq", 0, 0, tiled=True
    )
    grad_inputs = (1.0 - alpha_attn) * grad_one + jnp.sum(
        tokens_terms.astype(jnp.float32), axis=0
    )

    def team_spread(part):
        whole = jnp.zeros((dp_count, TEAM, ff_part), jnp.float32)
        return lax.dynamic_update_slice_in_dim(
            whole, part.reshape(dp_count, 1, ff_part), team_rank, 1
        ).reshape(ff_width)

    grad_s_qk = lax.dynamic_update_slice_in_dim(
        jnp.zeros((model_width,), jnp.float32), grad_head_gain.reshape(-1), offset, 0
    )
    small_terms = (
        grad_s_qk,
        team_spread(grad_s_u),
        team_spread(grad_s_v),
        grad_alpha_attn,
        grad_alpha_mlp,
    )
    packed = jnp.concatenate(
        [term.reshape(dp_count * seq_count, -1) for term in small_terms], axis=1
    )
    packed = lax.psum_scatter(packed, ("dp", "seq"), scatter_dimension=0, tiled=True).reshape(-1)
    small_shards = []
    spot = 0
    for term in small_terms:
        width = term.shape[0] // (dp_count * seq_count)
        small_shards.append(packed[spot : spot + width])
        spot += width
    return (
        output,
        grad_inputs.reshape(tokens.shape),
        shard_w_qkv,
        shard_w_attn_out,
        shard_w_in,
        shard_w_down,
    ) + tuple(small_shards)


def solution(mesh):
    placed = (
        P("dp", "seq", None),
        P("dp", None),
        P("dp", None),
        P("dp", None),
        P("dp", None),
        P("dp", None),
        P(),
        P(),
        P(),
        P(),
        P(),
        P("dp", "seq", None),
    )
    return jax.shard_map(
        body,
        mesh=mesh,
        in_specs=placed,
        out_specs=(
            P("dp", "seq", None),
            P("dp", "seq", None),
            P(("dp", "seq"), None),
            P(("dp", "seq"), None),
            P(("dp", "seq"), None),
            P(("dp", "seq"), None),
            P(("dp", "seq")),
            P(("dp", "seq")),
            P(("dp", "seq")),
            P(("dp", "seq")),
            P(("dp", "seq")),
        ),
        check_vma=False,
    )
```

```python
import functools
import math

import jax
import jax.numpy as jnp
from jax import lax
from jax.experimental import pallas as pl
from jax.experimental.pallas import tpu as pltpu
from jax.sharding import PartitionSpec as P

MESH_ID = pl.DeviceIdType.MESH
TEAM = 4

HEADS = 16
HD = 64


EPS = 1e-06
ROPE_BASE = 10000.0
MASKED_SCORE = -1e30


def rms_norm(values):
    inverse = lax.rsqrt(jnp.mean(values * values, axis=-1, keepdims=True) + EPS)
    return (values * inverse, inverse)


def rms_back(grad_in, normed, inverse):
    return inverse * (grad_in - normed * jnp.mean(grad_in * normed, axis=-1, keepdims=True))


def contract_rows(left_arr, right_arr):
    return lax.dot_general(
        left_arr, right_arr, (((0,), (0,)), ((), ())), preferred_element_type=jnp.float32
    )


def contract_cols(left_arr, right_arr):
    return lax.dot_general(
        left_arr, right_arr, (((1,), (1,)), ((), ())), preferred_element_type=jnp.float32
    )


def doc_positions(seg_row):
    length = seg_row.shape[0]
    places = jnp.arange(length, dtype=jnp.int32)
    is_start = jnp.concatenate([jnp.ones((1,), dtype=bool), seg_row[1:] != seg_row[:-1]])
    starts = lax.cummax(jnp.where(is_start, places, 0), axis=0)
    return (places - starts).astype(jnp.float32)


def rope_tables(positions, head_dim):
    half_dim = head_dim // 2
    inverse_freq = ROPE_BASE ** (-(jnp.arange(half_dim, dtype=jnp.float32) * 2.0 / head_dim))
    angles = positions[:, None] * inverse_freq[None, :]
    return (jnp.cos(angles)[:, None, :], jnp.sin(angles)[:, None, :])


def rotate(values, cosine, sine_tab):
    half_dim = values.shape[-1] // 2
    low_half = values[..., :half_dim]
    high_half = values[..., half_dim:]
    return jnp.concatenate(
        [low_half * cosine - high_half * sine_tab, high_half * cosine + low_half * sine_tab],
        axis=-1,
    )


def head_prep(head_raw, cosine, sine_tab, head_gain):
    rotated = rotate(head_raw.astype(jnp.float32), cosine, sine_tab)
    head_unit, inverse = rms_norm(rotated)
    return (head_unit, inverse, (head_unit * head_gain).astype(jnp.bfloat16))


def head_back(grad_n, head_unit, inverse, head_gain, cosine, sine_tab):
    grad_rot = rms_back(grad_n * head_gain, head_unit, inverse)
    return rotate(grad_rot, cosine, -sine_tab)


def allowed(seg_row, block_start, block_len):
    query_idx = block_start + jnp.arange(block_len, dtype=jnp.int32)
    key_idx = jnp.arange(seg_row.shape[0], dtype=jnp.int32)
    seg_query = lax.dynamic_slice_in_dim(seg_row, block_start, block_len)
    same_doc = seg_query[:, None] == seg_row[None, :]
    causal = key_idx[None, :] <= query_idx[:, None]
    not_padding = (seg_query[:, None] != 0) | (key_idx[None, :] == query_idx[:, None])
    return causal & same_doc & not_padding


def attend_forward(query_n, key_n, value_b, seg_row, score_scale):
    length, groups, head_dim = query_n.shape
    block_len = min(512, length)
    block_count = length // block_len
    query_blocks = query_n.reshape(block_count, block_len, groups, head_dim)
    starts = jnp.arange(block_count, dtype=jnp.int32) * block_len

    def one_block(block_in):
        query_part, block_start = block_in
        scores = (
            jnp.einsum("qhd,khd->hqk", query_part, key_n, preferred_element_type=jnp.float32)
            * score_scale
        )
        mask_ok = allowed(seg_row, block_start, block_len)
        scores = jnp.where(mask_ok[None], scores, MASKED_SCORE)
        row_max = jnp.max(scores, axis=-1, keepdims=True)
        weights_exp = jnp.exp(scores - row_max)
        row_total = jnp.sum(weights_exp, axis=-1, keepdims=True)
        attn_probs = (weights_exp / row_total).astype(jnp.bfloat16)
        attn_part = jnp.einsum(
            "hqk,khd->qhd", attn_probs, value_b, preferred_element_type=jnp.float32
        )
        return (attn_part.astype(jnp.bfloat16), (row_max + jnp.log(row_total))[..., 0])

    attn_mixed, log_sums = lax.map(one_block, (query_blocks, starts))
    return (attn_mixed.reshape(length, groups * head_dim), log_sums)


def attend_backward(query_n, key_n, value_b, grad_attn, log_sums, seg_row, score_scale):
    length, groups, head_dim = query_n.shape
    block_len = min(512, length)
    block_count = length // block_len
    query_blocks = query_n.reshape(block_count, block_len, groups, head_dim)
    grad_blocks = grad_attn.reshape(block_count, block_len, groups, head_dim)
    starts = jnp.arange(block_count, dtype=jnp.int32) * block_len

    def one_block(accums, block_in):
        key_acc, value_acc = accums
        query_part, grad_part, lse_part, block_start = block_in
        scores = (
            jnp.einsum("qhd,khd->hqk", query_part, key_n, preferred_element_type=jnp.float32)
            * score_scale
        )
        mask_ok = allowed(seg_row, block_start, block_len)
        attn_probs = jnp.where(mask_ok[None], jnp.exp(scores - lse_part[..., None]), 0.0)
        grad_probs = jnp.einsum(
            "qhd,khd->hqk", grad_part, value_b, preferred_element_type=jnp.float32
        )
        delta_row = jnp.sum(grad_probs * attn_probs, axis=-1, keepdims=True)
        grad_scores = (attn_probs * (grad_probs - delta_row)).astype(jnp.bfloat16)
        grad_query = (
            jnp.einsum("hqk,khd->qhd", grad_scores, key_n, preferred_element_type=jnp.float32)
            * score_scale
        )
        key_acc = (
            key_acc
            + jnp.einsum(
                "hqk,qhd->khd", grad_scores, query_part, preferred_element_type=jnp.float32
            )
            * score_scale
        )
        value_acc = value_acc + jnp.einsum(
            "hqk,qhd->khd",
            attn_probs.astype(jnp.bfloat16),
            grad_part,
            preferred_element_type=jnp.float32,
        )
        return ((key_acc, value_acc), grad_query)

    zeros_init = jnp.zeros((length, groups, head_dim), jnp.float32)
    (grad_key, grad_value), grad_query = lax.scan(
        one_block, (zeros_init, zeros_init), (query_blocks, grad_blocks, log_sums, starts)
    )
    return (grad_query.reshape(length, groups, head_dim), grad_key, grad_value)


def greet(peers):
    barrier = pltpu.get_barrier_semaphore()
    for peer in peers:
        pl.semaphore_signal(barrier, inc=1, device_id=peer, device_id_type=MESH_ID)
    pl.semaphore_wait(barrier, len(peers))


def flip(place, bit):
    return place + bit - 2 * bit * lax.rem(place // bit, 2)


def seq_gather_kernel(count, own_ref, out_ref, send_sem, recv_sem, local_sem):
    rows = own_ref.shape[0]
    mine = lax.axis_index("seq")
    peers = [lax.rem(mine + step, count) for step in range(1, count)]
    greet([{"seq": peer} for peer in peers])
    spot = pl.ds(pl.multiple_of(mine * rows, rows), rows)
    copies = []
    for slot, peer in enumerate(peers):
        copies.append(
            pltpu.make_async_remote_copy(
                src_ref=own_ref,
                dst_ref=out_ref.at[spot],
                send_sem=send_sem.at[slot],
                recv_sem=recv_sem.at[slot],
                device_id={"seq": peer},
                device_id_type=MESH_ID,
            )
        )
    for copy in copies:
        copy.start()
    local = pltpu.make_async_copy(own_ref, out_ref.at[spot], local_sem)
    local.start()
    local.wait()
    for copy in copies:
        copy.wait()


def seq_gather(own):
    count = lax.axis_size("seq")
    rows, width = own.shape
    return pl.pallas_call(
        functools.partial(seq_gather_kernel, count),
        out_shape=jax.ShapeDtypeStruct((count * rows, width), own.dtype),
        in_specs=[pl.BlockSpec(memory_space=pl.ANY)],
        out_specs=pl.BlockSpec(memory_space=pl.ANY),
        scratch_shapes=[
            pltpu.SemaphoreType.DMA((count - 1,)),
            pltpu.SemaphoreType.DMA((count - 1,)),
            pltpu.SemaphoreType.DMA,
        ],
        cost_estimate=pl.CostEstimate(
            flops=0, bytes_accessed=100 * count * rows * width, transcendentals=0
        ),
        compiler_params=pltpu.CompilerParams(collective_id=0, has_side_effects=True),
    )(own)


PIECES = 4


def team_gather_kernel(own_ref, out_ref, send_sem, recv_sem, local_sem):
    rows = own_ref.shape[0]
    piece = rows // PIECES
    place = lax.axis_index("dp")
    far, near = flip(place, 2), flip(place, 1)
    rank, far_rank = lax.rem(place, TEAM), lax.rem(far, TEAM)
    greet([{"dp": far}, {"dp": near}])

    def spot(owner, index):
        return out_ref.at[pl.ds(pl.multiple_of(owner * rows + index * piece, piece), piece)]

    def push(source, owner, index, kind, peer):
        return pltpu.make_async_remote_copy(
            src_ref=source,
            dst_ref=spot(owner, index),
            send_sem=send_sem.at[kind, index],
            recv_sem=recv_sem.at[kind, index],
            device_id={"dp": peer},
            device_id_type=MESH_ID,
        )

    across = [push(own_ref.at[pl.ds(i * piece, piece)], rank, i, 0, far) for i in range(PIECES)]
    beside = [push(own_ref.at[pl.ds(i * piece, piece)], rank, i, 1, near) for i in range(PIECES)]
    for copy in across:
        copy.start()
    for copy in beside:
        copy.start()
    local = pltpu.make_async_copy(
        own_ref, out_ref.at[pl.ds(pl.multiple_of(rank * rows, rows), rows)], local_sem
    )
    local.start()
    passed = [push(spot(far_rank, i), far_rank, i, 2, near) for i in range(PIECES)]
    for i in range(PIECES):
        across[i].wait_recv()
        passed[i].start()
    local.wait()
    for copy in across:
        copy.wait_send()
    for copy in beside:
        copy.wait()
    for copy in passed:
        copy.wait()


def team_gather(own):
    rows, width = own.shape
    return pl.pallas_call(
        team_gather_kernel,
        out_shape=jax.ShapeDtypeStruct((TEAM * rows, width), own.dtype),
        in_specs=[pl.BlockSpec(memory_space=pl.ANY)],
        out_specs=pl.BlockSpec(memory_space=pl.ANY),
        scratch_shapes=[
            pltpu.SemaphoreType.DMA((3, PIECES)),
            pltpu.SemaphoreType.DMA((3, PIECES)),
            pltpu.SemaphoreType.DMA,
        ],
        cost_estimate=pl.CostEstimate(
            flops=0, bytes_accessed=50 * TEAM * rows * width, transcendentals=0
        ),
        compiler_params=pltpu.CompilerParams(collective_id=1, has_side_effects=True),
    )(own)


def team_sum_kernel(part_ref, out_ref, near_buf, send_buf, far_buf, send_sem, recv_sem, far_send, far_recv):
    rows = out_ref.shape[0]
    piece = rows // PIECES
    place = lax.axis_index("dp")
    far, near = flip(place, 2), flip(place, 1)
    rank, far_rank = lax.rem(place, TEAM), lax.rem(far, TEAM)
    near_rank = lax.rem(near, TEAM)
    cross_rank = lax.rem(flip(near, 2), TEAM)
    greet([{"dp": far}, {"dp": near}])

    def to_near(owner, slot, index):
        return pltpu.make_async_remote_copy(
            src_ref=part_ref.at[owner, pl.ds(index * piece, piece)],
            dst_ref=near_buf.at[slot, pl.ds(index * piece, piece)],
            send_sem=send_sem.at[slot, index],
            recv_sem=recv_sem.at[slot, index],
            device_id={"dp": near},
            device_id_type=MESH_ID,
        )

    outward = [to_near(cross_rank, 0, i) for i in range(PIECES)]
    inward = [to_near(near_rank, 1, i) for i in range(PIECES)]
    for copy in outward + inward:
        copy.start()
    ships = []
    for i in range(PIECES):
        here = pl.ds(i * piece, piece)
        outward[i].wait_recv()
        send_buf[here] = (
            part_ref[far_rank, here].astype(jnp.float32) + near_buf[0, here].astype(jnp.float32)
        ).astype(send_buf.dtype)
        ships.append(
            pltpu.make_async_remote_copy(
                src_ref=send_buf.at[here],
                dst_ref=far_buf.at[here],
                send_sem=far_send.at[i],
                recv_sem=far_recv.at[i],
                device_id={"dp": far},
                device_id_type=MESH_ID,
            )
        )
        if i > 0:
            ships[i - 1].start()
    for i in range(PIECES):
        here = pl.ds(i * piece, piece)
        inward[i].wait_recv()
        out_ref[here] = part_ref[rank, here].astype(jnp.float32) + near_buf[1, here].astype(
            jnp.float32
        )
        if i == 0:
            ships[PIECES - 1].start()
    for i in range(PIECES):
        here = pl.ds(i * piece, piece)
        ships[i].wait_recv()
        out_ref[here] = out_ref[here] + far_buf[here].astype(jnp.float32)
    for copy in outward + inward + ships:
        copy.wait_send()


def team_sum(part):
    _, rows, width = part.shape
    return pl.pallas_call(
        team_sum_kernel,
        out_shape=jax.ShapeDtypeStruct((rows, width), jnp.float32),
        in_specs=[pl.BlockSpec(memory_space=pltpu.VMEM)],
        out_specs=pl.BlockSpec(memory_space=pltpu.VMEM),
        scratch_shapes=[
            pltpu.VMEM((2, rows, width), part.dtype),
            pltpu.VMEM((rows, width), part.dtype),
            pltpu.VMEM((rows, width), part.dtype),
            pltpu.SemaphoreType.DMA((2, PIECES)),
            pltpu.SemaphoreType.DMA((2, PIECES)),
            pltpu.SemaphoreType.DMA((PIECES,)),
            pltpu.SemaphoreType.DMA((PIECES,)),
        ],
        cost_estimate=pl.CostEstimate(
            flops=0, bytes_accessed=50 * TEAM * rows * width, transcendentals=0
        ),
        compiler_params=pltpu.CompilerParams(collective_id=2, has_side_effects=True),
    )(part)


def seq_swap_kernel(to_tokens, count, part_ref, out_ref, send_sem, recv_sem, local_sem):
    rows = part_ref.shape[0] // count if to_tokens else part_ref.shape[0]
    width = part_ref.shape[1] if to_tokens else part_ref.shape[1] // count
    mine = lax.axis_index("seq")
    peers = [lax.rem(mine + step, count) for step in range(1, count)]
    greet([{"seq": peer} for peer in peers])

    def by_rows(ref, index):
        return ref.at[pl.ds(pl.multiple_of(index * rows, rows), rows), :]

    def by_columns(ref, index):
        return ref.at[:, pl.ds(pl.multiple_of(index * width, width), width)]

    take, give = (by_rows, by_columns) if to_tokens else (by_columns, by_rows)
    copies = [
        pltpu.make_async_remote_copy(
            src_ref=take(part_ref, peer),
            dst_ref=give(out_ref, mine),
            send_sem=send_sem.at[slot],
            recv_sem=recv_sem.at[slot],
            device_id={"seq": peer},
            device_id_type=MESH_ID,
        )
        for slot, peer in enumerate(peers)
    ]
    for copy in copies:
        copy.start()
    local = pltpu.make_async_copy(take(part_ref, mine), give(out_ref, mine), local_sem)
    local.start()
    local.wait()
    for copy in copies:
        copy.wait()


def seq_swap(part, to_tokens):
    count = lax.axis_size("seq")
    rows, width = part.shape
    shape = (rows // count, width * count) if to_tokens else (rows * count, width // count)
    return pl.pallas_call(
        functools.partial(seq_swap_kernel, to_tokens, count),
        out_shape=jax.ShapeDtypeStruct(shape, part.dtype),
        in_specs=[pl.BlockSpec(memory_space=pltpu.VMEM)],
        out_specs=pl.BlockSpec(memory_space=pltpu.VMEM),
        scratch_shapes=[
            pltpu.SemaphoreType.DMA((count - 1,)),
            pltpu.SemaphoreType.DMA((count - 1,)),
            pltpu.SemaphoreType.DMA,
        ],
        cost_estimate=pl.CostEstimate(
            flops=0, bytes_accessed=100 * rows * width, transcendentals=0
        ),
        compiler_params=pltpu.CompilerParams(
            collective_id=3 if to_tokens else 4, has_side_effects=True
        ),
    )(part)


def seq_sum_kernel(count, part_ref, base_ref, out_ref, landed, send_sem, recv_sem):
    mine = lax.axis_index("seq")
    peers = [lax.rem(mine + step, count) for step in range(1, count)]
    greet([{"seq": peer} for peer in peers])
    copies = [
        pltpu.make_async_remote_copy(
            src_ref=part_ref.at[peer],
            dst_ref=landed.at[slot],
            send_sem=send_sem.at[slot],
            recv_sem=recv_sem.at[slot],
            device_id={"seq": peer},
            device_id_type=MESH_ID,
        )
        for slot, peer in enumerate(peers)
    ]
    for copy in copies:
        copy.start()
    out_ref[...] = base_ref[...] + part_ref[mine].astype(jnp.float32)
    for slot, copy in enumerate(copies):
        copy.wait_recv()
        out_ref[...] = out_ref[...] + landed[slot].astype(jnp.float32)
    for copy in copies:
        copy.wait_send()


def seq_sum(part, base):
    count, rows, width = part.shape
    return pl.pallas_call(
        functools.partial(seq_sum_kernel, count),
        out_shape=jax.ShapeDtypeStruct((rows, width), jnp.float32),
        in_specs=[pl.BlockSpec(memory_space=pltpu.VMEM)] * 2,
        out_specs=pl.BlockSpec(memory_space=pltpu.VMEM),
        scratch_shapes=[
            pltpu.VMEM((count - 1, rows, width), part.dtype),
            pltpu.SemaphoreType.DMA((count - 1,)),
            pltpu.SemaphoreType.DMA((count - 1,)),
        ],
        cost_estimate=pl.CostEstimate(
            flops=0, bytes_accessed=100 * count * rows * width, transcendentals=0
        ),
        compiler_params=pltpu.CompilerParams(collective_id=5, has_side_effects=True),
    )(part, base)


def pack_kernel(in_ref, down_ref, in_out, down_out):
    depth = down_out.shape[1]
    places = in_out.shape[0]
    for rank in range(TEAM):
        for part in range(in_out.shape[2] // depth):
            first = (part * TEAM + rank) * depth
            values = in_ref[:, first : first + depth]
            for place in range(rank, places, TEAM):
                in_out[place, :, part * depth : (part + 1) * depth] = values
        values = down_ref[rank * depth : (rank + 1) * depth, :]
        for place in range(rank, places, TEAM):
            down_out[place] = values


def pack_ff(w_in, w_down, dp_count, ff_part):
    in_rows, in_cols = w_in.shape
    model_width = w_down.shape[1]
    if ff_part % 128 == 0 and in_rows == ff_part:
        return pl.pallas_call(
            pack_kernel,
            out_shape=(
                jax.ShapeDtypeStruct((dp_count, in_rows, in_cols // TEAM), w_in.dtype),
                jax.ShapeDtypeStruct((dp_count, ff_part, model_width), w_in.dtype),
            ),
            in_specs=[pl.BlockSpec(memory_space=pltpu.VMEM)] * 2,
            out_specs=(
                pl.BlockSpec(memory_space=pltpu.VMEM),
                pl.BlockSpec(memory_space=pltpu.VMEM),
            ),
            cost_estimate=pl.CostEstimate(flops=0, bytes_accessed=1 << 23, transcendentals=0),
        )(w_in, w_down)
    copies = dp_count // TEAM
    in_parts = w_in.reshape(in_rows, 2 * dp_count, TEAM, ff_part).transpose(2, 0, 1, 3)
    in_blocks = jnp.concatenate([in_parts.reshape(TEAM, in_rows, in_cols // TEAM)] * copies)
    down_blocks = jnp.concatenate([w_down.reshape(TEAM, ff_part, model_width)] * copies)
    return in_blocks, down_blocks


def body(
    tokens,
    segments,
    w_qkv,
    w_attn_out,
    w_in,
    w_down,
    s_qk,
    s_u,
    s_v,
    alpha_attn,
    alpha_mlp,
    cotangent,
):
    model_width = tokens.shape[-1]
    inputs_b = tokens.reshape(-1, model_width)
    inputs_f = inputs_b.astype(jnp.float32)
    seg_row = segments.reshape(-1)
    length = seg_row.shape[0]
    local_rows = inputs_b.shape[0]
    seq_count = lax.axis_size("seq")
    dp_count = lax.axis_size("dp")
    head_group = HEADS // seq_count
    group_width = head_group * HD
    seq_rank = lax.axis_index("seq")
    team_rank = lax.rem(lax.axis_index("dp"), TEAM)
    offset = seq_rank * group_width
    head_gain = lax.dynamic_slice_in_dim(s_qk, offset, group_width).reshape(head_group, HD)
    score_scale = 1.0 / math.sqrt(HD)
    ff_width = s_u.shape[0]
    ff_part = ff_width // dp_count // TEAM
    ff_team = ff_width // TEAM
    in_rows = w_in.shape[0]

    head_cols = lax.dynamic_slice_in_dim(
        w_qkv.reshape(-1, 3, model_width), offset, group_width, axis=2
    ).reshape(-1, 3 * group_width)
    gathered = lax.all_gather(
        jnp.concatenate([head_cols, w_attn_out], axis=1), "dp", axis=0, tiled=True
    )
    heads_qkv = gathered[:, : 3 * group_width]
    full_out = gathered[:, 3 * group_width :]
    in_blocks, down_blocks = pack_ff(w_in, w_down, dp_count, ff_part)
    seq_tokens = seq_gather(inputs_b)
    in_blocks, down_blocks, seq_tokens = lax.optimization_barrier(
        (in_blocks, down_blocks, seq_tokens)
    )
    team_in = lax.all_to_all(in_blocks, "dp", 0, 0, tiled=True)
    team_down = lax.all_to_all(down_blocks, "dp", 0, 0, tiled=True)
    team_in = team_in.reshape(model_width, 2 * ff_team)
    team_down = team_down.reshape(ff_team, model_width)

    def team_slice(scale):
        return lax.dynamic_index_in_dim(
            scale.reshape(dp_count, TEAM, ff_part), team_rank, 1, keepdims=False
        ).reshape(ff_team)

    s_u_team, s_v_team = team_slice(s_u), team_slice(s_v)

    by_heads = (
        jnp.dot(seq_tokens, heads_qkv, preferred_element_type=jnp.float32)
        .astype(jnp.bfloat16)
        .reshape(length, 3, group_width)
    )
    cosine, sine_tab = rope_tables(doc_positions(seg_row), HD)
    query_unit, query_inv, query_n = head_prep(
        by_heads[:, 0].reshape(length, head_group, HD), cosine, sine_tab, head_gain
    )
    key_unit, key_inv, key_n = head_prep(
        by_heads[:, 1].reshape(length, head_group, HD), cosine, sine_tab, head_gain
    )
    value_b = by_heads[:, 2].reshape(length, head_group, HD)
    attn_mixed, log_sums = attend_forward(query_n, key_n, value_b, seg_row, score_scale)
    attn_pieces = seq_swap(attn_mixed, True)
    attn_proj = jnp.dot(attn_pieces, full_out, preferred_element_type=jnp.float32)
    attn_unit, attn_inv = rms_norm(attn_proj)
    hidden, hidden_inv = rms_norm(inputs_f + alpha_attn * (attn_unit - inputs_f))
    hidden_b = hidden.astype(jnp.bfloat16)

    team_hidden = team_gather(hidden_b)
    up_gate = jnp.dot(team_hidden, team_in, preferred_element_type=jnp.float32)
    up_raw = up_gate[:, :ff_team]
    gate_raw = up_gate[:, ff_team:]
    up_val = s_u_team * up_raw
    gate_val = s_v_team * gate_raw
    gate_sig = jax.nn.sigmoid(gate_val)
    silu_gate = gate_val * gate_sig
    inner_act = (silu_gate * up_val).astype(jnp.bfloat16)
    down_part = jnp.dot(inner_act, team_down, preferred_element_type=jnp.float32)
    down_proj = team_sum(down_part.astype(jnp.bfloat16).reshape(TEAM, local_rows, model_width))
    mlp_unit, mlp_inv = rms_norm(down_proj)
    result, result_inv = rms_norm(hidden + alpha_mlp * (mlp_unit - hidden))
    output = result.astype(jnp.bfloat16).reshape(tokens.shape)
    grad_res = cotangent.reshape(-1, model_width).astype(jnp.float32)
    grad_two = rms_back(grad_res, result, result_inv)
    grad_alpha_mlp = jnp.sum(grad_two * (mlp_unit - hidden), axis=0)
    grad_down_proj = rms_back(alpha_mlp * grad_two, mlp_unit, mlp_inv).astype(jnp.bfloat16)

    team_grad = team_gather(grad_down_proj)
    grad_inner = contract_cols(team_grad, team_down)
    grad_up_val = grad_inner * silu_gate
    grad_gate_val = grad_inner * up_val * gate_sig * (1.0 + gate_val * (1.0 - gate_sig))
    grad_s_u = jnp.sum(grad_up_val * up_raw, axis=0)
    grad_s_v = jnp.sum(grad_gate_val * gate_raw, axis=0)
    grad_up_gate = jnp.concatenate(
        [grad_up_val * s_u_team, grad_gate_val * s_v_team], axis=1
    ).astype(jnp.bfloat16)
    hidden_part = contract_cols(grad_up_gate, team_in)
    hidden_sum = team_sum(hidden_part.astype(jnp.bfloat16).reshape(TEAM, local_rows, model_width))
    grad_hidden = (1.0 - alpha_mlp) * grad_two + hidden_sum
    in_terms = contract_rows(team_hidden, grad_up_gate).astype(jnp.bfloat16)
    down_terms = contract_rows(inner_act, team_grad).astype(jnp.bfloat16)
    ff_terms = jnp.concatenate(
        [
            in_terms[:, :ff_team].reshape(dp_count, in_rows, ff_team),
            in_terms[:, ff_team:].reshape(dp_count, in_rows, ff_team),
            down_terms.reshape(dp_count, in_rows, model_width),
        ],
        axis=1,
    )
    ff_terms = lax.all_to_all(ff_terms, "dp", 0, 0, tiled=True)
    ff_sums = jnp.sum(
        ff_terms.reshape(dp_count // TEAM, TEAM, 3, in_rows, model_width).astype(jnp.float32),
        axis=0,
    ).astype(jnp.bfloat16)
    out_rows = in_rows // seq_count
    in_sums = (
        ff_sums[:, :2]
        .reshape(TEAM, 2, seq_count, out_rows, model_width)
        .transpose(2, 0, 1, 3, 4)
        .reshape(seq_count, TEAM * 2 * out_rows, model_width)
    )
    down_sums = ff_sums[:, 2].reshape(seq_count, -1, model_width)

    grad_one = rms_back(grad_hidden, hidden, hidden_inv)
    grad_alpha_attn = jnp.sum(grad_one * (attn_unit - inputs_f), axis=0)
    grad_attn_proj = rms_back(alpha_attn * grad_one, attn_unit, attn_inv).astype(jnp.bfloat16)
    grad_pieces = contract_cols(grad_attn_proj, full_out).astype(jnp.bfloat16)
    grad_w_attn_out = contract_rows(attn_pieces, grad_attn_proj).astype(jnp.bfloat16)
    out_sums = lax.psum_scatter(
        grad_w_attn_out, "dp", scatter_dimension=0, tiled=True
    ).reshape(seq_count, out_rows, model_width)
    shards = lax.psum_scatter(
        jnp.concatenate([in_sums, down_sums, out_sums], axis=1).reshape(-1, model_width),
        "seq",
        scatter_dimension=0,
        tiled=True,
    )
    in_span = TEAM * 2 * out_rows
    shard_w_in = (
        shards[:in_span]
        .reshape(TEAM, 2, out_rows, dp_count, ff_part)
        .transpose(2, 1, 3, 0, 4)
        .reshape(out_rows, 2 * ff_width)
        .astype(jnp.float32)
    )
    shard_w_down = shards[in_span:-out_rows].astype(jnp.float32)
    shard_w_attn_out = shards[-out_rows:].astype(jnp.float32)
    grad_heads = seq_swap(grad_pieces, False).reshape(length, head_group, HD)
    grad_query_n, grad_key_n, grad_value = attend_backward(
        query_n, key_n, value_b, grad_heads, log_sums, seg_row, score_scale
    )
    grad_head_gain = jnp.sum(grad_query_n * query_unit + grad_key_n * key_unit, axis=0)
    grad_query = head_back(grad_query_n, query_unit, query_inv, head_gain, cosine, sine_tab)
    grad_key = head_back(grad_key_n, key_unit, key_inv, head_gain, cosine, sine_tab)
    grad_qkv = (
        jnp.stack([grad_query, grad_key, grad_value], axis=1)
        .reshape(length, 3 * group_width)
        .astype(jnp.bfloat16)
    )

    def team_spread(part):
        whole = jnp.zeros((dp_count, TEAM, ff_part), jnp.float32)
        return lax.dynamic_update_slice_in_dim(
            whole, part.reshape(dp_count, 1, ff_part), team_rank, 1
        ).reshape(ff_width)

    grad_s_qk = lax.dynamic_update_slice_in_dim(
        jnp.zeros((model_width,), jnp.float32), grad_head_gain.reshape(-1), offset, 0
    )
    small_terms = (
        grad_s_qk,
        team_spread(grad_s_u),
        team_spread(grad_s_v),
        grad_alpha_attn,
        grad_alpha_mlp,
    )
    grad_w_qkv = contract_rows(seq_tokens, grad_qkv).astype(jnp.bfloat16)
    small_count = sum(term.shape[0] for term in small_terms) // (dp_count * seq_count)
    small_rows = 8 * -(-small_count // (24 * group_width))
    packed = jnp.concatenate(
        [term.reshape(dp_count, seq_count, -1) for term in small_terms], axis=2
    ).astype(jnp.bfloat16)
    packed = jnp.pad(packed, ((0, 0), (0, 0), (0, small_rows * 3 * group_width - small_count)))
    packed = jnp.concatenate(
        [
            grad_w_qkv.reshape(dp_count, seq_count, out_rows, 3 * group_width),
            packed.reshape(dp_count, seq_count, small_rows, 3 * group_width),
        ],
        axis=2,
    )
    span = out_rows + small_rows
    packed = lax.psum_scatter(
        packed.reshape(dp_count * seq_count * span, 3 * group_width),
        "dp",
        scatter_dimension=0,
        tiled=True,
    )
    tokens_part = contract_cols(grad_qkv, heads_qkv).astype(jnp.bfloat16)
    grad_inputs = seq_sum(
        tokens_part.reshape(seq_count, local_rows, model_width), (1.0 - alpha_attn) * grad_one
    )
    packed = lax.all_to_all(
        packed.reshape(seq_count, span, 3 * group_width), "seq", 0, 0, tiled=True
    )
    shard_w_qkv = (
        packed[:, :out_rows]
        .reshape(seq_count, -1, 3, group_width)
        .transpose(1, 2, 0, 3)
        .reshape(-1, 3 * model_width)
        .astype(jnp.float32)
    )
    packed = jnp.sum(packed[:, out_rows:].astype(jnp.float32), axis=0).reshape(-1)
    small_shards = []
    spot = 0
    for term in small_terms:
        width = term.shape[0] // (dp_count * seq_count)
        small_shards.append(packed[spot : spot + width])
        spot += width
    return (
        output,
        grad_inputs.reshape(tokens.shape),
        shard_w_qkv,
        shard_w_attn_out,
        shard_w_in,
        shard_w_down,
    ) + tuple(small_shards)


def solution(mesh):
    placed = (
        P("dp", "seq", None),
        P("dp", None),
        P("dp", None),
        P("dp", None),
        P("dp", None),
        P("dp", None),
        P(),
        P(),
        P(),
        P(),
        P(),
        P("dp", "seq", None),
    )

    return jax.shard_map(
        body,
        mesh=mesh,
        in_specs=placed,
        out_specs=(
            P("dp", "seq", None),
            P("dp", "seq", None),
            P(("dp", "seq"), None),
            P(("dp", "seq"), None),
            P(("dp", "seq"), None),
            P(("dp", "seq"), None),
            P(("dp", "seq")),
            P(("dp", "seq")),
            P(("dp", "seq")),
            P(("dp", "seq")),
            P(("dp", "seq")),
        ),
        check_vma=False,
    )
```

```python
import functools
import math

import jax
import jax.numpy as jnp
from jax import lax
from jax.experimental import pallas as pl
from jax.experimental.pallas import tpu as pltpu
from jax.sharding import PartitionSpec as P

MESH_ID = pl.DeviceIdType.MESH
TEAM = 4

HEADS = 16
HD = 64


EPS = 1e-06
ROPE_BASE = 10000.0
MASKED_SCORE = -1e30


def rms_norm(values):
    inverse = lax.rsqrt(jnp.mean(values * values, axis=-1, keepdims=True) + EPS)
    return (values * inverse, inverse)


def rms_back(grad_in, normed, inverse):
    return inverse * (grad_in - normed * jnp.mean(grad_in * normed, axis=-1, keepdims=True))


def contract_rows(left_arr, right_arr):
    return lax.dot_general(
        left_arr, right_arr, (((0,), (0,)), ((), ())), preferred_element_type=jnp.float32
    )


def contract_cols(left_arr, right_arr):
    return lax.dot_general(
        left_arr, right_arr, (((1,), (1,)), ((), ())), preferred_element_type=jnp.float32
    )


def doc_positions(seg_row):
    length = seg_row.shape[0]
    places = jnp.arange(length, dtype=jnp.int32)
    is_start = jnp.concatenate([jnp.ones((1,), dtype=bool), seg_row[1:] != seg_row[:-1]])
    starts = lax.cummax(jnp.where(is_start, places, 0), axis=0)
    return (places - starts).astype(jnp.float32)


def rope_tables(positions, head_dim):
    half_dim = head_dim // 2
    inverse_freq = ROPE_BASE ** (-(jnp.arange(half_dim, dtype=jnp.float32) * 2.0 / head_dim))
    angles = positions[:, None] * inverse_freq[None, :]
    return (jnp.cos(angles)[:, None, :], jnp.sin(angles)[:, None, :])


def rotate(values, cosine, sine_tab):
    half_dim = values.shape[-1] // 2
    low_half = values[..., :half_dim]
    high_half = values[..., half_dim:]
    return jnp.concatenate(
        [low_half * cosine - high_half * sine_tab, high_half * cosine + low_half * sine_tab],
        axis=-1,
    )


def head_prep(head_raw, cosine, sine_tab, head_gain):
    rotated = rotate(head_raw.astype(jnp.float32), cosine, sine_tab)
    head_unit, inverse = rms_norm(rotated)
    return (head_unit, inverse, (head_unit * head_gain).astype(jnp.bfloat16))


def head_back(grad_n, head_unit, inverse, head_gain, cosine, sine_tab):
    grad_rot = rms_back(grad_n * head_gain, head_unit, inverse)
    return rotate(grad_rot, cosine, -sine_tab)


QUERY_BLOCK = 256


def block_probs(query_part, key_part, key_seg, query_seg, first, score_scale):
    rows = query_part.shape[0]
    span = key_part.shape[0]
    scores = contract_cols(key_part, query_part) * score_scale
    key_idx = lax.broadcasted_iota(jnp.int32, (span, rows), 0)
    query_idx = first + lax.broadcasted_iota(jnp.int32, (span, rows), 1)
    open_seg = jnp.where(query_seg == 0, -1, query_seg)
    allowed = ((key_seg == open_seg) & (key_idx <= query_idx)) | (key_idx == query_idx)
    scores = jnp.where(allowed, scores, MASKED_SCORE)
    weights_exp = jnp.exp(scores - jnp.max(scores, axis=0, keepdims=True))
    return weights_exp * (1.0 / jnp.sum(weights_exp, axis=0, keepdims=True))


def flip_f32(values):
    return values.astype(jnp.float32).T


def attn_forward_kernel(score_scale, query_ref, key_ref, value_ref, col_ref, row_ref, out_ref):
    length, width = query_ref.shape
    for head in range(width // HD):
        lanes = slice(head * HD, (head + 1) * HD)
        key_all = key_ref[:, lanes]
        value_t = flip_f32(value_ref[:, lanes]).astype(jnp.bfloat16)
        for first in range(0, length, QUERY_BLOCK):
            span = first + QUERY_BLOCK
            probs = block_probs(
                query_ref[first:span, lanes],
                key_all[:span],
                col_ref[:span],
                row_ref[:, first:span],
                first,
                score_scale,
            ).astype(jnp.bfloat16)
            mixed = jnp.dot(value_t[:, :span], probs, preferred_element_type=jnp.float32)
            out_ref[first:span, lanes] = mixed.T.astype(out_ref.dtype)


def attn_backward_kernel(
    score_scale,
    query_ref,
    key_ref,
    value_ref,
    grad_ref,
    col_ref,
    row_ref,
    query_out,
    key_out,
    value_out,
):
    length, width = query_ref.shape
    for head in range(width // HD):
        lanes = slice(head * HD, (head + 1) * HD)
        key_all = key_ref[:, lanes]
        value_all = value_ref[:, lanes]
        key_t = flip_f32(key_all).astype(jnp.bfloat16)
        for first in range(length - QUERY_BLOCK, -1, -QUERY_BLOCK):
            span = first + QUERY_BLOCK
            query_part = query_ref[first:span, lanes]
            grad_part = grad_ref[first:span, lanes]
            probs = block_probs(
                query_part,
                key_all[:span],
                col_ref[:span],
                row_ref[:, first:span],
                first,
                score_scale,
            )
            grad_value = jnp.dot(
                probs.astype(jnp.bfloat16), grad_part, preferred_element_type=jnp.float32
            )
            grad_probs = contract_cols(value_all[:span], grad_part)
            delta = jnp.sum(grad_probs * probs, axis=0, keepdims=True)
            grad_scores = (probs * (grad_probs - delta)).astype(jnp.bfloat16)
            grad_key = (
                jnp.dot(grad_scores, query_part, preferred_element_type=jnp.float32) * score_scale
            )
            grad_query = (
                jnp.dot(key_t[:, :span], grad_scores, preferred_element_type=jnp.float32)
                * score_scale
            )
            query_out[first:span, lanes] = grad_query.T
            if span == length:
                key_out[:, lanes] = grad_key
                value_out[:, lanes] = grad_value
            else:
                key_out[:span, lanes] += grad_key
                value_out[:span, lanes] += grad_value


def attn_call(kernel, score_scale, arrays, seg_row, outs):
    length, width = arrays[0].shape
    pair = min(2 * HD, width)
    block = pl.BlockSpec((length, pair), lambda i: (0, i))
    work = length * length * width
    return pl.pallas_call(
        functools.partial(kernel, score_scale),
        grid=(width // pair,),
        out_shape=[jax.ShapeDtypeStruct((length, width), dtype) for dtype in outs],
        in_specs=[block] * len(arrays)
        + [
            pl.BlockSpec((length, 1), lambda i: (0, 0)),
            pl.BlockSpec((1, length), lambda i: (0, 0)),
        ],
        out_specs=[block] * len(outs),
        cost_estimate=pl.CostEstimate(
            flops=24 * work * len(outs), bytes_accessed=8 * length * width, transcendentals=0
        ),
        compiler_params=pltpu.CompilerParams(vmem_limit_bytes=48 << 20),
    )(*arrays, seg_row.reshape(length, 1), seg_row.reshape(1, length))


def attend_forward(query_n, key_n, value_b, seg_row, score_scale):
    return attn_call(
        attn_forward_kernel, score_scale, (query_n, key_n, value_b), seg_row, (jnp.bfloat16,)
    )[0]


def attend_backward(query_n, key_n, value_b, grad_attn, seg_row, score_scale):
    return attn_call(
        attn_backward_kernel,
        score_scale,
        (query_n, key_n, value_b, grad_attn),
        seg_row,
        (jnp.float32,) * 3,
    )


def greet(peers):
    barrier = pltpu.get_barrier_semaphore()
    for peer in peers:
        pl.semaphore_signal(barrier, inc=1, device_id=peer, device_id_type=MESH_ID)
    pl.semaphore_wait(barrier, len(peers))


def flip(place, bit):
    return place + bit - 2 * bit * lax.rem(place // bit, 2)


def seq_gather_kernel(count, own_ref, out_ref, send_sem, recv_sem, local_sem):
    rows = own_ref.shape[0]
    mine = lax.axis_index("seq")
    peers = [lax.rem(mine + step, count) for step in range(1, count)]
    greet([{"seq": peer} for peer in peers])
    spot = pl.ds(pl.multiple_of(mine * rows, rows), rows)
    copies = []
    for slot, peer in enumerate(peers):
        copies.append(
            pltpu.make_async_remote_copy(
                src_ref=own_ref,
                dst_ref=out_ref.at[spot],
                send_sem=send_sem.at[slot],
                recv_sem=recv_sem.at[slot],
                device_id={"seq": peer},
                device_id_type=MESH_ID,
            )
        )
    for copy in copies:
        copy.start()
    local = pltpu.make_async_copy(own_ref, out_ref.at[spot], local_sem)
    local.start()
    local.wait()
    for copy in copies:
        copy.wait()


def seq_gather(own):
    count = lax.axis_size("seq")
    rows, width = own.shape
    return pl.pallas_call(
        functools.partial(seq_gather_kernel, count),
        out_shape=jax.ShapeDtypeStruct((count * rows, width), own.dtype),
        in_specs=[pl.BlockSpec(memory_space=pl.ANY)],
        out_specs=pl.BlockSpec(memory_space=pl.ANY),
        scratch_shapes=[
            pltpu.SemaphoreType.DMA((count - 1,)),
            pltpu.SemaphoreType.DMA((count - 1,)),
            pltpu.SemaphoreType.DMA,
        ],
        cost_estimate=pl.CostEstimate(
            flops=0, bytes_accessed=100 * count * rows * width, transcendentals=0
        ),
        compiler_params=pltpu.CompilerParams(collective_id=0, has_side_effects=True),
    )(own)


PIECES = 4


def team_gather_kernel(own_ref, out_ref, send_sem, recv_sem, local_sem):
    rows = own_ref.shape[0]
    piece = rows // PIECES
    place = lax.axis_index("dp")
    far, near = flip(place, 2), flip(place, 1)
    rank, far_rank = lax.rem(place, TEAM), lax.rem(far, TEAM)
    greet([{"dp": far}, {"dp": near}])

    def spot(owner, index):
        return out_ref.at[pl.ds(pl.multiple_of(owner * rows + index * piece, piece), piece)]

    def push(source, owner, index, kind, peer):
        return pltpu.make_async_remote_copy(
            src_ref=source,
            dst_ref=spot(owner, index),
            send_sem=send_sem.at[kind, index],
            recv_sem=recv_sem.at[kind, index],
            device_id={"dp": peer},
            device_id_type=MESH_ID,
        )

    across = [push(own_ref.at[pl.ds(i * piece, piece)], rank, i, 0, far) for i in range(PIECES)]
    beside = [push(own_ref.at[pl.ds(i * piece, piece)], rank, i, 1, near) for i in range(PIECES)]
    for copy in across:
        copy.start()
    for copy in beside:
        copy.start()
    local = pltpu.make_async_copy(
        own_ref, out_ref.at[pl.ds(pl.multiple_of(rank * rows, rows), rows)], local_sem
    )
    local.start()
    passed = [push(spot(far_rank, i), far_rank, i, 2, near) for i in range(PIECES)]
    for i in range(PIECES):
        across[i].wait_recv()
        passed[i].start()
    local.wait()
    for copy in across:
        copy.wait_send()
    for copy in beside:
        copy.wait()
    for copy in passed:
        copy.wait()


def team_gather(own):
    rows, width = own.shape
    return pl.pallas_call(
        team_gather_kernel,
        out_shape=jax.ShapeDtypeStruct((TEAM * rows, width), own.dtype),
        in_specs=[pl.BlockSpec(memory_space=pl.ANY)],
        out_specs=pl.BlockSpec(memory_space=pl.ANY),
        scratch_shapes=[
            pltpu.SemaphoreType.DMA((3, PIECES)),
            pltpu.SemaphoreType.DMA((3, PIECES)),
            pltpu.SemaphoreType.DMA,
        ],
        cost_estimate=pl.CostEstimate(
            flops=0, bytes_accessed=50 * TEAM * rows * width, transcendentals=0
        ),
        compiler_params=pltpu.CompilerParams(collective_id=1, has_side_effects=True),
    )(own)


def team_sum_kernel(part_ref, out_ref, near_buf, send_buf, far_buf, send_sem, recv_sem, far_send, far_recv):
    rows = out_ref.shape[0]
    piece = rows // PIECES
    place = lax.axis_index("dp")
    far, near = flip(place, 2), flip(place, 1)
    rank, far_rank = lax.rem(place, TEAM), lax.rem(far, TEAM)
    near_rank = lax.rem(near, TEAM)
    cross_rank = lax.rem(flip(near, 2), TEAM)
    greet([{"dp": far}, {"dp": near}])

    def to_near(owner, slot, index):
        return pltpu.make_async_remote_copy(
            src_ref=part_ref.at[owner, pl.ds(index * piece, piece)],
            dst_ref=near_buf.at[slot, pl.ds(index * piece, piece)],
            send_sem=send_sem.at[slot, index],
            recv_sem=recv_sem.at[slot, index],
            device_id={"dp": near},
            device_id_type=MESH_ID,
        )

    outward = [to_near(cross_rank, 0, i) for i in range(PIECES)]
    inward = [to_near(near_rank, 1, i) for i in range(PIECES)]
    for copy in outward + inward:
        copy.start()
    ships = []
    for i in range(PIECES):
        here = pl.ds(i * piece, piece)
        outward[i].wait_recv()
        send_buf[here] = (
            part_ref[far_rank, here].astype(jnp.float32) + near_buf[0, here].astype(jnp.float32)
        ).astype(send_buf.dtype)
        ships.append(
            pltpu.make_async_remote_copy(
                src_ref=send_buf.at[here],
                dst_ref=far_buf.at[here],
                send_sem=far_send.at[i],
                recv_sem=far_recv.at[i],
                device_id={"dp": far},
                device_id_type=MESH_ID,
            )
        )
        if i > 0:
            ships[i - 1].start()
    for i in range(PIECES):
        here = pl.ds(i * piece, piece)
        inward[i].wait_recv()
        out_ref[here] = part_ref[rank, here].astype(jnp.float32) + near_buf[1, here].astype(
            jnp.float32
        )
        if i == 0:
            ships[PIECES - 1].start()
    for i in range(PIECES):
        here = pl.ds(i * piece, piece)
        ships[i].wait_recv()
        out_ref[here] = out_ref[here] + far_buf[here].astype(jnp.float32)
    for copy in outward + inward + ships:
        copy.wait_send()


def team_sum(part):
    _, rows, width = part.shape
    return pl.pallas_call(
        team_sum_kernel,
        out_shape=jax.ShapeDtypeStruct((rows, width), jnp.float32),
        in_specs=[pl.BlockSpec(memory_space=pltpu.VMEM)],
        out_specs=pl.BlockSpec(memory_space=pltpu.VMEM),
        scratch_shapes=[
            pltpu.VMEM((2, rows, width), part.dtype),
            pltpu.VMEM((rows, width), part.dtype),
            pltpu.VMEM((rows, width), part.dtype),
            pltpu.SemaphoreType.DMA((2, PIECES)),
            pltpu.SemaphoreType.DMA((2, PIECES)),
            pltpu.SemaphoreType.DMA((PIECES,)),
            pltpu.SemaphoreType.DMA((PIECES,)),
        ],
        cost_estimate=pl.CostEstimate(
            flops=0, bytes_accessed=50 * TEAM * rows * width, transcendentals=0
        ),
        compiler_params=pltpu.CompilerParams(collective_id=2, has_side_effects=True),
    )(part)


def seq_swap_kernel(to_tokens, count, part_ref, out_ref, send_sem, recv_sem, local_sem):
    rows = part_ref.shape[0] // count if to_tokens else part_ref.shape[0]
    width = part_ref.shape[1] if to_tokens else part_ref.shape[1] // count
    mine = lax.axis_index("seq")
    peers = [lax.rem(mine + step, count) for step in range(1, count)]
    greet([{"seq": peer} for peer in peers])

    def by_rows(ref, index):
        return ref.at[pl.ds(pl.multiple_of(index * rows, rows), rows), :]

    def by_columns(ref, index):
        return ref.at[:, pl.ds(pl.multiple_of(index * width, width), width)]

    take, give = (by_rows, by_columns) if to_tokens else (by_columns, by_rows)
    copies = [
        pltpu.make_async_remote_copy(
            src_ref=take(part_ref, peer),
            dst_ref=give(out_ref, mine),
            send_sem=send_sem.at[slot],
            recv_sem=recv_sem.at[slot],
            device_id={"seq": peer},
            device_id_type=MESH_ID,
        )
        for slot, peer in enumerate(peers)
    ]
    for copy in copies:
        copy.start()
    local = pltpu.make_async_copy(take(part_ref, mine), give(out_ref, mine), local_sem)
    local.start()
    local.wait()
    for copy in copies:
        copy.wait()


def seq_swap(part, to_tokens):
    count = lax.axis_size("seq")
    rows, width = part.shape
    shape = (rows // count, width * count) if to_tokens else (rows * count, width // count)
    return pl.pallas_call(
        functools.partial(seq_swap_kernel, to_tokens, count),
        out_shape=jax.ShapeDtypeStruct(shape, part.dtype),
        in_specs=[pl.BlockSpec(memory_space=pltpu.VMEM)],
        out_specs=pl.BlockSpec(memory_space=pltpu.VMEM),
        scratch_shapes=[
            pltpu.SemaphoreType.DMA((count - 1,)),
            pltpu.SemaphoreType.DMA((count - 1,)),
            pltpu.SemaphoreType.DMA,
        ],
        cost_estimate=pl.CostEstimate(
            flops=0, bytes_accessed=100 * rows * width, transcendentals=0
        ),
        compiler_params=pltpu.CompilerParams(
            collective_id=3 if to_tokens else 4, has_side_effects=True
        ),
    )(part)


def seq_sum_kernel(count, part_ref, base_ref, out_ref, landed, send_sem, recv_sem):
    mine = lax.axis_index("seq")
    peers = [lax.rem(mine + step, count) for step in range(1, count)]
    greet([{"seq": peer} for peer in peers])
    copies = [
        pltpu.make_async_remote_copy(
            src_ref=part_ref.at[peer],
            dst_ref=landed.at[slot],
            send_sem=send_sem.at[slot],
            recv_sem=recv_sem.at[slot],
            device_id={"seq": peer},
            device_id_type=MESH_ID,
        )
        for slot, peer in enumerate(peers)
    ]
    for copy in copies:
        copy.start()
    out_ref[...] = base_ref[...] + part_ref[mine].astype(jnp.float32)
    for slot, copy in enumerate(copies):
        copy.wait_recv()
        out_ref[...] = out_ref[...] + landed[slot].astype(jnp.float32)
    for copy in copies:
        copy.wait_send()


def seq_sum(part, base):
    count, rows, width = part.shape
    return pl.pallas_call(
        functools.partial(seq_sum_kernel, count),
        out_shape=jax.ShapeDtypeStruct((rows, width), jnp.float32),
        in_specs=[pl.BlockSpec(memory_space=pltpu.VMEM)] * 2,
        out_specs=pl.BlockSpec(memory_space=pltpu.VMEM),
        scratch_shapes=[
            pltpu.VMEM((count - 1, rows, width), part.dtype),
            pltpu.SemaphoreType.DMA((count - 1,)),
            pltpu.SemaphoreType.DMA((count - 1,)),
        ],
        cost_estimate=pl.CostEstimate(
            flops=0, bytes_accessed=100 * count * rows * width, transcendentals=0
        ),
        compiler_params=pltpu.CompilerParams(collective_id=5, has_side_effects=True),
    )(part, base)


def pack_kernel(in_ref, down_ref, in_out, down_out):
    depth = down_out.shape[1]
    places = in_out.shape[0]
    for rank in range(TEAM):
        for part in range(in_out.shape[2] // depth):
            first = (part * TEAM + rank) * depth
            values = in_ref[:, first : first + depth]
            for place in range(rank, places, TEAM):
                in_out[place, :, part * depth : (part + 1) * depth] = values
        values = down_ref[rank * depth : (rank + 1) * depth, :]
        for place in range(rank, places, TEAM):
            down_out[place] = values


def pack_ff(w_in, w_down, dp_count, ff_part):
    in_rows, in_cols = w_in.shape
    model_width = w_down.shape[1]
    if ff_part % 128 == 0 and in_rows == ff_part:
        return pl.pallas_call(
            pack_kernel,
            out_shape=(
                jax.ShapeDtypeStruct((dp_count, in_rows, in_cols // TEAM), w_in.dtype),
                jax.ShapeDtypeStruct((dp_count, ff_part, model_width), w_in.dtype),
            ),
            in_specs=[pl.BlockSpec(memory_space=pltpu.VMEM)] * 2,
            out_specs=(
                pl.BlockSpec(memory_space=pltpu.VMEM),
                pl.BlockSpec(memory_space=pltpu.VMEM),
            ),
            cost_estimate=pl.CostEstimate(flops=0, bytes_accessed=1 << 23, transcendentals=0),
        )(w_in, w_down)
    copies = dp_count // TEAM
    in_parts = w_in.reshape(in_rows, 2 * dp_count, TEAM, ff_part).transpose(2, 0, 1, 3)
    in_blocks = jnp.concatenate([in_parts.reshape(TEAM, in_rows, in_cols // TEAM)] * copies)
    down_blocks = jnp.concatenate([w_down.reshape(TEAM, ff_part, model_width)] * copies)
    return in_blocks, down_blocks


def body(
    tokens,
    segments,
    w_qkv,
    w_attn_out,
    w_in,
    w_down,
    s_qk,
    s_u,
    s_v,
    alpha_attn,
    alpha_mlp,
    cotangent,
):
    model_width = tokens.shape[-1]
    inputs_b = tokens.reshape(-1, model_width)
    inputs_f = inputs_b.astype(jnp.float32)
    seg_row = segments.reshape(-1)
    length = seg_row.shape[0]
    local_rows = inputs_b.shape[0]
    seq_count = lax.axis_size("seq")
    dp_count = lax.axis_size("dp")
    head_group = HEADS // seq_count
    group_width = head_group * HD
    seq_rank = lax.axis_index("seq")
    team_rank = lax.rem(lax.axis_index("dp"), TEAM)
    offset = seq_rank * group_width
    head_gain = lax.dynamic_slice_in_dim(s_qk, offset, group_width).reshape(head_group, HD)
    score_scale = 1.0 / math.sqrt(HD)
    ff_width = s_u.shape[0]
    ff_part = ff_width // dp_count // TEAM
    ff_team = ff_width // TEAM
    in_rows = w_in.shape[0]

    head_cols = lax.dynamic_slice_in_dim(
        w_qkv.reshape(-1, 3, model_width), offset, group_width, axis=2
    ).reshape(-1, 3 * group_width)
    gathered = lax.all_gather(
        jnp.concatenate([head_cols, w_attn_out], axis=1), "dp", axis=0, tiled=True
    )
    heads_qkv = gathered[:, : 3 * group_width]
    full_out = gathered[:, 3 * group_width :]
    in_blocks, down_blocks = pack_ff(w_in, w_down, dp_count, ff_part)
    seq_tokens = seq_gather(inputs_b)
    in_blocks, down_blocks, seq_tokens = lax.optimization_barrier(
        (in_blocks, down_blocks, seq_tokens)
    )
    team_in = lax.all_to_all(in_blocks, "dp", 0, 0, tiled=True)
    team_down = lax.all_to_all(down_blocks, "dp", 0, 0, tiled=True)
    team_in = team_in.reshape(model_width, 2 * ff_team)
    team_down = team_down.reshape(ff_team, model_width)

    def team_slice(scale):
        return lax.dynamic_index_in_dim(
            scale.reshape(dp_count, TEAM, ff_part), team_rank, 1, keepdims=False
        ).reshape(ff_team)

    s_u_team, s_v_team = team_slice(s_u), team_slice(s_v)

    by_heads = (
        jnp.dot(seq_tokens, heads_qkv, preferred_element_type=jnp.float32)
        .astype(jnp.bfloat16)
        .reshape(length, 3, group_width)
    )
    cosine, sine_tab = rope_tables(doc_positions(seg_row), HD)
    query_unit, query_inv, query_n = head_prep(
        by_heads[:, 0].reshape(length, head_group, HD), cosine, sine_tab, head_gain
    )
    key_unit, key_inv, key_n = head_prep(
        by_heads[:, 1].reshape(length, head_group, HD), cosine, sine_tab, head_gain
    )
    query_n = query_n.reshape(length, group_width)
    key_n = key_n.reshape(length, group_width)
    value_b = by_heads[:, 2]
    attn_mixed = attend_forward(query_n, key_n, value_b, seg_row, score_scale)
    attn_pieces = seq_swap(attn_mixed, True)
    attn_proj = jnp.dot(attn_pieces, full_out, preferred_element_type=jnp.float32)
    attn_unit, attn_inv = rms_norm(attn_proj)
    hidden, hidden_inv = rms_norm(inputs_f + alpha_attn * (attn_unit - inputs_f))
    hidden_b = hidden.astype(jnp.bfloat16)

    team_hidden = team_gather(hidden_b)
    up_gate = jnp.dot(team_hidden, team_in, preferred_element_type=jnp.float32)
    up_raw = up_gate[:, :ff_team]
    gate_raw = up_gate[:, ff_team:]
    up_val = s_u_team * up_raw
    gate_val = s_v_team * gate_raw
    gate_sig = jax.nn.sigmoid(gate_val)
    silu_gate = gate_val * gate_sig
    inner_act = (silu_gate * up_val).astype(jnp.bfloat16)
    down_part = jnp.dot(inner_act, team_down, preferred_element_type=jnp.float32)
    down_proj = team_sum(down_part.astype(jnp.bfloat16).reshape(TEAM, local_rows, model_width))
    mlp_unit, mlp_inv = rms_norm(down_proj)
    result, result_inv = rms_norm(hidden + alpha_mlp * (mlp_unit - hidden))
    output = result.astype(jnp.bfloat16).reshape(tokens.shape)
    grad_res = cotangent.reshape(-1, model_width).astype(jnp.float32)
    grad_two = rms_back(grad_res, result, result_inv)
    grad_alpha_mlp = jnp.sum(grad_two * (mlp_unit - hidden), axis=0)
    grad_down_proj = rms_back(alpha_mlp * grad_two, mlp_unit, mlp_inv).astype(jnp.bfloat16)

    team_grad = team_gather(grad_down_proj)
    grad_inner = contract_cols(team_grad, team_down)
    grad_up_val = grad_inner * silu_gate
    grad_gate_val = grad_inner * up_val * gate_sig * (1.0 + gate_val * (1.0 - gate_sig))
    grad_s_u = jnp.sum(grad_up_val * up_raw, axis=0)
    grad_s_v = jnp.sum(grad_gate_val * gate_raw, axis=0)
    grad_up_gate = jnp.concatenate(
        [grad_up_val * s_u_team, grad_gate_val * s_v_team], axis=1
    ).astype(jnp.bfloat16)
    hidden_part = contract_cols(grad_up_gate, team_in)
    hidden_sum = team_sum(hidden_part.astype(jnp.bfloat16).reshape(TEAM, local_rows, model_width))
    in_terms = contract_rows(team_hidden, grad_up_gate).astype(jnp.bfloat16)
    down_terms = contract_rows(inner_act, team_grad).astype(jnp.bfloat16)
    ff_terms = jnp.concatenate(
        [
            in_terms[:, :ff_team].reshape(dp_count, in_rows, ff_team),
            in_terms[:, ff_team:].reshape(dp_count, in_rows, ff_team),
            down_terms.reshape(dp_count, in_rows, model_width),
        ],
        axis=1,
    )
    ff_terms, hidden_sum = lax.optimization_barrier((ff_terms, hidden_sum))
    grad_hidden = (1.0 - alpha_mlp) * grad_two + hidden_sum
    ff_terms = lax.all_to_all(ff_terms, "dp", 0, 0, tiled=True)
    ff_sums = jnp.sum(
        ff_terms.reshape(dp_count // TEAM, TEAM, 3, in_rows, model_width).astype(jnp.float32),
        axis=0,
    ).astype(jnp.bfloat16)
    out_rows = in_rows // seq_count
    in_sums = (
        ff_sums[:, :2]
        .reshape(TEAM, 2, seq_count, out_rows, model_width)
        .transpose(2, 0, 1, 3, 4)
        .reshape(seq_count, TEAM * 2 * out_rows, model_width)
    )
    down_sums = ff_sums[:, 2].reshape(seq_count, -1, model_width)

    grad_one = rms_back(grad_hidden, hidden, hidden_inv)
    grad_alpha_attn = jnp.sum(grad_one * (attn_unit - inputs_f), axis=0)
    grad_attn_proj = rms_back(alpha_attn * grad_one, attn_unit, attn_inv).astype(jnp.bfloat16)
    grad_pieces = contract_cols(grad_attn_proj, full_out).astype(jnp.bfloat16)
    grad_w_attn_out = contract_rows(attn_pieces, grad_attn_proj).astype(jnp.bfloat16)
    out_sums = lax.psum_scatter(
        grad_w_attn_out, "dp", scatter_dimension=0, tiled=True
    ).reshape(seq_count, out_rows, model_width)
    shards = lax.psum_scatter(
        jnp.concatenate([in_sums, down_sums, out_sums], axis=1).reshape(-1, model_width),
        "seq",
        scatter_dimension=0,
        tiled=True,
    )
    in_span = TEAM * 2 * out_rows
    shard_w_in = (
        shards[:in_span]
        .reshape(TEAM, 2, out_rows, dp_count, ff_part)
        .transpose(2, 1, 3, 0, 4)
        .reshape(out_rows, 2 * ff_width)
        .astype(jnp.float32)
    )
    shard_w_down = shards[in_span:-out_rows].astype(jnp.float32)
    shard_w_attn_out = shards[-out_rows:].astype(jnp.float32)
    grad_heads = seq_swap(grad_pieces, False)
    grad_query_n, grad_key_n, grad_value = attend_backward(
        query_n, key_n, value_b, grad_heads, seg_row, score_scale
    )
    grad_query_n = grad_query_n.reshape(length, head_group, HD)
    grad_key_n = grad_key_n.reshape(length, head_group, HD)
    grad_value = grad_value.reshape(length, head_group, HD)
    grad_head_gain = jnp.sum(grad_query_n * query_unit + grad_key_n * key_unit, axis=0)
    grad_query = head_back(grad_query_n, query_unit, query_inv, head_gain, cosine, sine_tab)
    grad_key = head_back(grad_key_n, key_unit, key_inv, head_gain, cosine, sine_tab)
    grad_qkv = (
        jnp.stack([grad_query, grad_key, grad_value], axis=1)
        .reshape(length, 3 * group_width)
        .astype(jnp.bfloat16)
    )

    def team_spread(part):
        whole = jnp.zeros((dp_count, TEAM, ff_part), jnp.float32)
        return lax.dynamic_update_slice_in_dim(
            whole, part.reshape(dp_count, 1, ff_part), team_rank, 1
        ).reshape(ff_width)

    grad_s_qk = lax.dynamic_update_slice_in_dim(
        jnp.zeros((model_width,), jnp.float32), grad_head_gain.reshape(-1), offset, 0
    )
    small_terms = (
        grad_s_qk,
        team_spread(grad_s_u),
        team_spread(grad_s_v),
        grad_alpha_attn,
        grad_alpha_mlp,
    )
    grad_w_qkv = contract_rows(seq_tokens, grad_qkv).astype(jnp.bfloat16)
    small_count = sum(term.shape[0] for term in small_terms) // (dp_count * seq_count)
    small_rows = 8 * -(-small_count // (24 * group_width))
    packed = jnp.concatenate(
        [term.reshape(dp_count, seq_count, -1) for term in small_terms], axis=2
    ).astype(jnp.bfloat16)
    packed = jnp.pad(packed, ((0, 0), (0, 0), (0, small_rows * 3 * group_width - small_count)))
    packed = jnp.concatenate(
        [
            grad_w_qkv.reshape(dp_count, seq_count, out_rows, 3 * group_width),
            packed.reshape(dp_count, seq_count, small_rows, 3 * group_width),
        ],
        axis=2,
    )
    span = out_rows + small_rows
    packed = lax.psum_scatter(
        packed.reshape(dp_count * seq_count * span, 3 * group_width),
        "dp",
        scatter_dimension=0,
        tiled=True,
    )
    tokens_part = contract_cols(grad_qkv, heads_qkv).astype(jnp.bfloat16)
    grad_inputs = seq_sum(
        tokens_part.reshape(seq_count, local_rows, model_width), (1.0 - alpha_attn) * grad_one
    )
    packed = lax.all_to_all(
        packed.reshape(seq_count, span, 3 * group_width), "seq", 0, 0, tiled=True
    )
    shard_w_qkv = (
        packed[:, :out_rows]
        .reshape(seq_count, -1, 3, group_width)
        .transpose(1, 2, 0, 3)
        .reshape(-1, 3 * model_width)
        .astype(jnp.float32)
    )
    packed = jnp.sum(packed[:, out_rows:].astype(jnp.float32), axis=0).reshape(-1)
    small_shards = []
    spot = 0
    for term in small_terms:
        width = term.shape[0] // (dp_count * seq_count)
        small_shards.append(packed[spot : spot + width])
        spot += width
    return (
        output,
        grad_inputs.reshape(tokens.shape),
        shard_w_qkv,
        shard_w_attn_out,
        shard_w_in,
        shard_w_down,
    ) + tuple(small_shards)


def solution(mesh):
    placed = (
        P("dp", "seq", None),
        P("dp", None),
        P("dp", None),
        P("dp", None),
        P("dp", None),
        P("dp", None),
        P(),
        P(),
        P(),
        P(),
        P(),
        P("dp", "seq", None),
    )

    return jax.shard_map(
        body,
        mesh=mesh,
        in_specs=placed,
        out_specs=(
            P("dp", "seq", None),
            P("dp", "seq", None),
            P(("dp", "seq"), None),
            P(("dp", "seq"), None),
            P(("dp", "seq"), None),
            P(("dp", "seq"), None),
            P(("dp", "seq")),
            P(("dp", "seq")),
            P(("dp", "seq")),
            P(("dp", "seq")),
            P(("dp", "seq")),
        ),
        check_vma=False,
    )
```
